256 devices in a mesh: atom: 32 (over z, x_hi, core), kvec: 8 (over x_lo, y).
Axes of the slice: x: 4 (x_hi: 2, x_lo: 2; x = x_hi * 2 + x_lo), y: 4, z: 8, core: 2. Of those that a mesh axis runs over, the one named last changes fastest.
Arguments:
- scaled_coordinate_array: float32 [3, 524288], P(None, 'atom'), may hold values from 0 to 1
- particle_charge_list: float32 [524288], P('atom'), may hold values from -4 to 4
- reciprocal_triples: int32 [3, 4096], P(None, 'kvec'), may hold values from -128 to 128, as said below
Outputs:
- forces: float32 [3, 524288], P(None, 'atom')
- potential: float32 [524288], P('atom')
- energy: float32 [], replicated
The draws below stay inside these ranges and needn't reach their ends.
Inputs may be any that keep to these rules, and one draw needn't show every extreme that they name: `reciprocal_triples`: every k-vector has a component of magnitude 64 or more.
All inputs are finite; a program needn't handle non-finite values.
Results may differ from the reference program's by a relative error of at most 0.0003.
Values sent between devices are 32-bit elements; how exact they have to be, the bound alone decides.
No kernel may reach another device: no remote copies, remote signals or barrier semaphores. Data moves between devices by JAX's collectives and lax.ppermute only.
A program may use at most 192 MiB of HBM per device.

```python
import math
import jax
import jax.numpy as jnp
from jax import lax

NK = 4096
NATOMS = 524288


def draw_reciprocal_triples(key, part):
    first_key, second_key, third_key, fourth_key = jax.random.split(key, 4)
    component_values = jax.random.randint(first_key, (3, NK), -128, 129, dtype=jnp.int32)
    facing_axis = jax.random.randint(second_key, (NK,), 0, 3, dtype=jnp.int32)
    magnitude = jax.random.randint(third_key, (NK,), 64, 129, dtype=jnp.int32)
    polarity = jax.random.randint(fourth_key, (NK,), 0, 2, dtype=jnp.int32) * 2 - 1
    chosen = jnp.arange(3, dtype=jnp.int32)[:, None] == facing_axis[None, :]
    return jnp.where(chosen, (magnitude * polarity)[None, :], component_values).astype(jnp.int32)


def block_levels(key, dims, pieces, least, largest):
    factor_of = 1.0
    for dim, parts in pieces:
        heights = jax.random.uniform(jax.random.fold_in(jax.random.fold_in(key, 6), dim), (parts,), jnp.float32, least / len(pieces), largest / len(pieces))
        factor_of = factor_of * jnp.repeat(jnp.exp(heights), dims[dim] // parts).reshape((-1,) + (1,) * (len(dims) - 1 - dim))
    return factor_of


def centred(rng, dims, spread, bound, pieces=(), kind=jnp.bfloat16):
    loudness = block_levels(rng, dims, pieces, -0.22, 0.18) if pieces else 1.0
    values = jax.random.normal(rng, dims, jnp.float32) * spread * loudness
    return jnp.minimum(jnp.maximum(values, -bound), bound).astype(kind)


def setup_inputs(seed: int = 0) -> dict:
    arg_keys = jax.random.split(jax.random.key(seed), 4)
    return {
        "scaled_coordinate_array": jnp.clip(1.0 * jax.random.uniform(arg_keys[0], (3, NATOMS), jnp.float32) ** block_levels(arg_keys[0], (3, NATOMS), ((1, 32),), -0.2, 0.2), 0.0, 1.0),
        "particle_charge_list": centred(arg_keys[1], (NATOMS,), 1.0, 4.0, ((0, 32),), jnp.float32),
        "reciprocal_triples": draw_reciprocal_triples(jax.random.fold_in(arg_keys[3], 71), 0),
    }


def mode_energy_terms(reciprocal_triples):
    reciprocal_direction_table = 2.0 * math.pi * reciprocal_triples.astype(jnp.float32)
    reciprocal_norm_squared = lax.optimization_barrier(jnp.sum(reciprocal_direction_table * reciprocal_direction_table, axis=0))
    gaussian_screening_weight = 4.0 * math.pi * jnp.exp(-reciprocal_norm_squared / 1600000.0) / reciprocal_norm_squared
    return (reciprocal_direction_table, gaussian_screening_weight)

def phase_angle(packed, reciprocal_direction_table):
    angle = packed[0][:, None] * reciprocal_direction_table[0][None, :]
    angle = angle + packed[1][:, None] * reciprocal_direction_table[1][None, :]
    return angle + packed[2][:, None] * reciprocal_direction_table[2][None, :]

def reference(scaled_coordinate_array, particle_charge_list, reciprocal_triples):
    reciprocal_direction_table, gaussian_screening_weight = mode_energy_terms(reciprocal_triples)
    natoms = scaled_coordinate_array.shape[1]
    packed = jnp.concatenate([scaled_coordinate_array, particle_charge_list[None, :]], axis=0)
    block = 2048 if natoms % 2048 == 0 else natoms
    blocks = packed.reshape(4, natoms // block, block).transpose(1, 0, 2)

    def gather_totals(totals, portion):
        angle = phase_angle(portion, reciprocal_direction_table)
        weights = portion[3][:, None]
        return ((totals[0] + lax.optimization_barrier(jnp.sum(weights * jnp.cos(angle), axis=0)), totals[1] + lax.optimization_barrier(jnp.sum(weights * jnp.sin(angle), axis=0))), None)
    zeros = jnp.zeros((reciprocal_direction_table.shape[1],), jnp.float32)
    (cosine_values, sine), unused = lax.scan(gather_totals, (zeros, zeros), blocks)
    energy = 50.0 / natoms * jnp.sum(gaussian_screening_weight * (cosine_values * cosine_values + sine * sine))
    weighted_cos = gaussian_screening_weight * cosine_values
    weighted_sin = gaussian_screening_weight * sine

    def respond(portion):
        angle = phase_angle(portion, reciprocal_direction_table)
        cos_tile = jnp.cos(angle)
        sin_tile = jnp.sin(angle)
        pot_raw = lax.optimization_barrier(jnp.sum(cos_tile * weighted_cos[None, :] + sin_tile * weighted_sin[None, :], axis=1))
        gradient = sin_tile * weighted_cos[None, :] - cos_tile * weighted_sin[None, :]
        rows = [lax.optimization_barrier(jnp.sum(gradient * reciprocal_direction_table[axis_id][None, :], axis=1)) for axis_id in range(3)]
        return jnp.stack(rows + [pot_raw], axis=0)
    result = lax.map(respond, blocks)
    result = result.transpose(1, 0, 2).reshape(4, natoms)
    scale = 1.0 / math.sqrt(natoms)
    forces = result[:3] * particle_charge_list[None, :] * scale
    potential = result[3] * (400.0 * scale)
    return (forces, potential, energy)
```

```python
import math

import jax
import jax.numpy as jnp
from jax import lax
from jax.experimental import pallas as pl
from jax.experimental.pallas import tpu as pltpu
from jax.sharding import PartitionSpec as P

TOP = 128
BLOCK = 2048
ROWS = BLOCK // 128
CHUNK = 128
MIB = 1 << 20


def phases_kernel(idx_ref, xyz_ref, q_ref, e_ref, s_ref, xc, xs, yc, ys, zc, zs, acc):
    b = pl.program_id(0)
    kc = pl.program_id(1)

    @pl.when((b == 0) & (kc == 0))
    def _():
        def clear(i, carry):
            acc[i] = jnp.zeros((8, 128), jnp.float32)
            return carry

        lax.fori_loop(0, acc.shape[0], clear, 0, unroll=8)

    @pl.when(kc == 0)
    def _():
        base = []
        for d in range(3):
            x = xyz_ref[d]
            angle = (2.0 * math.pi) * (x - jnp.round(x))
            base.append((jnp.cos(angle), jnp.sin(angle)))

        def put(h, state):
            (c0, s0), (c1, s1), (c2, s2) = state
            xc[h] = c0
            xs[h] = s0
            yc[h] = c1
            ys[TOP + h] = s1
            ys[TOP - h] = -s1
            zc[h] = c2
            zs[TOP + h] = s2
            zs[TOP - h] = -s2

        def step(h, state):
            put(h, state)
            return tuple(
                (c * bc - s * bs, c * bs + s * bc) for (c, s), (bc, bs) in zip(state, base)
            )

        one = jnp.ones((ROWS, 128), jnp.float32)
        zero = jnp.zeros((ROWS, 128), jnp.float32)
        put(0, ((one, zero),) * 3)
        lax.fori_loop(1, TOP + 1, step, tuple(base), unroll=4)

    q = q_ref[...]

    def mode(i, carry):
        k = kc * CHUNK + i
        h = idx_ref[0, k]
        cx, sx = xc[h], xs[h]
        cy, sy = yc[idx_ref[1, k]], ys[idx_ref[2, k]]
        cz, sz = zc[idx_ref[3, k]], zs[idx_ref[4, k]]
        cp = cx * cy - sx * sy
        sp = cx * sy + sx * cy
        c = cp * cz - sp * sz
        s = cp * sz + sp * cz
        e_ref[0, i, 0] = c
        e_ref[0, i, 1] = s
        qc = q * c
        qs = q * s
        acc[2 * k] += qc[:8] + qc[8:]
        acc[2 * k + 1] += qs[:8] + qs[8:]
        return carry

    lax.fori_loop(0, CHUNK, mode, 0, unroll=4)

    @pl.when((b == pl.num_programs(0) - 1) & (kc == pl.num_programs(1) - 1))
    def _():
        n = acc.shape[0]
        rows = acc[:, 0, :]
        for r in range(1, 8):
            rows = rows + acc[:, r, :]
        ones = jnp.ones((8, 128), jnp.float32)
        s_ref[...] = lax.dot_general(
            ones,
            rows,
            (((1,), (1,)), ((), ())),
            precision=lax.Precision.HIGHEST,
            preferred_element_type=jnp.float32,
        )


def response_kernel(w_ref, e_ref, o_ref):
    kc = pl.program_id(1)

    @pl.when(kc == 0)
    def _():
        o_ref[0, : 4 * ROWS] = jnp.zeros((4 * ROWS, 128), jnp.float32)
        o_ref[0, 4 * ROWS :] = jnp.full((8, 128), w_ref[5, 0], jnp.float32)

    def mode(i, carry):
        f0, f1, f2, p = carry
        k = kc * CHUNK + i
        wr, wi = w_ref[0, k], w_ref[1, k]
        c = e_ref[0, i, 0]
        s = e_ref[0, i, 1]
        p = p + (wr * c + wi * s)
        g = wr * s - wi * c
        return (f0 + w_ref[2, k] * g, f1 + w_ref[3, k] * g, f2 + w_ref[4, k] * g, p)

    start = tuple(o_ref[0, ROWS * c : ROWS * (c + 1)] for c in range(4))
    done = lax.fori_loop(0, CHUNK, mode, start, unroll=4)
    for c in range(4):
        o_ref[0, ROWS * c : ROWS * (c + 1)] = done[c]


def on_device(scaled_coordinate_array, particle_charge_list, reciprocal_triples):
    local_atoms = scaled_coordinate_array.shape[1]
    modes = reciprocal_triples.shape[1]
    n_atom = lax.axis_size("atom")
    n_kvec = lax.axis_size("kvec")
    natoms = local_atoms * n_atom
    blocks = local_atoms // BLOCK
    chunks = modes // CHUNK

    triples = reciprocal_triples * jnp.where(reciprocal_triples[0:1] < 0, -1, 1)
    table = 2.0 * math.pi * triples.astype(jnp.float32)
    norm = jnp.sum(table * table, axis=0)
    damping = 4.0 * math.pi * jnp.exp(-norm / 1600000.0) / norm
    idx = jnp.stack(
        [
            triples[0],
            jnp.abs(triples[1]),
            triples[1] + TOP,
            jnp.abs(triples[2]),
            triples[2] + TOP,
        ]
    )
    xyz = scaled_coordinate_array.reshape(3, local_atoms // 128, 128)
    q = particle_charge_list.reshape(local_atoms // 128, 128)

    e, s = pl.pallas_call(
        phases_kernel,
        grid=(blocks, chunks),
        in_specs=[
            pl.BlockSpec(memory_space=pltpu.SMEM),
            pl.BlockSpec((3, ROWS, 128), lambda b, c: (0, b, 0)),
            pl.BlockSpec((ROWS, 128), lambda b, c: (b, 0)),
        ],
        out_specs=[
            pl.BlockSpec((1, CHUNK, 2, ROWS, 128), lambda b, c: (b, c, 0, 0, 0)),
            pl.BlockSpec((8, 2 * modes), lambda b, c: (0, 0)),
        ],
        out_shape=[
            jax.ShapeDtypeStruct((blocks, modes, 2, ROWS, 128), jnp.float32),
            jax.ShapeDtypeStruct((8, 2 * modes), jnp.float32),
        ],
        scratch_shapes=[
            pltpu.VMEM((TOP + 1, ROWS, 128), jnp.float32),
            pltpu.VMEM((TOP + 1, ROWS, 128), jnp.float32),
            pltpu.VMEM((TOP + 1, ROWS, 128), jnp.float32),
            pltpu.VMEM((2 * TOP + 1, ROWS, 128), jnp.float32),
            pltpu.VMEM((TOP + 1, ROWS, 128), jnp.float32),
            pltpu.VMEM((2 * TOP + 1, ROWS, 128), jnp.float32),
            pltpu.VMEM((2 * modes, 8, 128), jnp.float32),
        ],
        compiler_params=pltpu.CompilerParams(
            dimension_semantics=("arbitrary", "arbitrary"), vmem_limit_bytes=40 * MIB
        ),
    )(idx, xyz, q)

    share = jnp.broadcast_to(s[0:1], (n_atom, 2 * modes))
    total = lax.all_to_all(share, "atom", 0, 0, tiled=True).sum(axis=0)
    total = total.reshape(modes, 2)
    cosine, sine = total[:, 0], total[:, 1]
    partial_energy = 50.0 / natoms * jnp.sum(damping * (cosine * cosine + sine * sine))
    w = jnp.concatenate(
        [
            (damping * cosine)[None],
            (damping * sine)[None],
            table,
            jnp.broadcast_to(partial_energy, (1, modes)),
        ]
    )

    terms = pl.pallas_call(
        response_kernel,
        grid=(blocks, chunks),
        in_specs=[
            pl.BlockSpec(memory_space=pltpu.SMEM),
            pl.BlockSpec((1, CHUNK, 2, ROWS, 128), lambda b, c: (b, c, 0, 0, 0)),
        ],
        out_specs=pl.BlockSpec((1, 4 * ROWS + 8, 128), lambda b, c: (b, 0, 0)),
        out_shape=jax.ShapeDtypeStruct((blocks, 4 * ROWS + 8, 128), jnp.float32),
        compiler_params=pltpu.CompilerParams(
            dimension_semantics=("arbitrary", "arbitrary"), vmem_limit_bytes=40 * MIB
        ),
    )(w, e)

    mine = lax.all_to_all(terms, "kvec", 0, 0, tiled=True).sum(axis=0)
    energy = mine[4 * ROWS, 0]
    copies = jnp.broadcast_to(mine[None, : 4 * ROWS], (n_kvec, 4 * ROWS, 128))
    summed = lax.all_to_all(copies, "kvec", 0, 0, tiled=True)
    summed = summed.reshape(n_kvec, 4, BLOCK).transpose(1, 0, 2).reshape(4, local_atoms)
    scale = 1.0 / math.sqrt(natoms)
    forces = summed[:3] * particle_charge_list[None, :] * scale
    potential = summed[3] * (400.0 * scale)
    return (forces, potential, energy)


def solution(mesh):
    return jax.shard_map(
        on_device,
        mesh=mesh,
        in_specs=(P(None, "atom"), P("atom"), P(None, "kvec")),
        out_specs=(P(None, "atom"), P("atom"), P()),
        check_vma=False,
    )
```

```python
import math

import jax
import jax.numpy as jnp
from jax import lax
from jax.experimental import pallas as pl
from jax.experimental.pallas import tpu as pltpu
from jax.sharding import PartitionSpec as P

TOP = 128
BLOCK = 4096
ROWS = BLOCK // 128
SPLIT = 4
PART = 32
CHUNK = SPLIT * PART
HALF = ROWS // 2
MIB = 1 << 20


def rows_of(ref, start):
    return ref[pl.ds(pl.multiple_of(start, ROWS), ROWS), :]


def phases_kernel(idx_ref, xyz_ref, q_ref, *refs):
    e_refs = refs[:SPLIT]
    s_ref, xc, xs, yc, ys, zc, zs, acc = refs[SPLIT:]
    b = pl.program_id(0)
    kc = pl.program_id(1)

    @pl.when((b == 0) & (kc == 0))
    def _():
        def clear(i, carry):
            acc[i] = jnp.zeros((8, 128), jnp.float32)
            return carry

        lax.fori_loop(0, acc.shape[0], clear, 0, unroll=8)

    @pl.when(kc == 0)
    def _():
        for part in range(2):
            low = part * HALF

            def row(h):
                return pl.ds(pl.multiple_of(h * ROWS + low, 8), HALF)

            base = []
            for d in range(3):
                x = xyz_ref[d, low : low + HALF]
                angle = (2.0 * math.pi) * (x - jnp.round(x))
                base.append((jnp.cos(angle), jnp.sin(angle)))

            def put(h, state):
                (c0, s0), (c1, s1), (c2, s2) = state
                xc[row(h)] = c0
                xs[row(h)] = s0
                yc[row(h)] = c1
                ys[row(TOP + h)] = s1
                ys[row(TOP - h)] = -s1
                zc[row(h)] = c2
                zs[row(TOP + h)] = s2
                zs[row(TOP - h)] = -s2

            def step(h, state):
                put(h, state)
                return tuple(
                    (c * bc - s * bs, c * bs + s * bc) for (c, s), (bc, bs) in zip(state, base)
                )

            one = jnp.ones((HALF, 128), jnp.float32)
            zero = jnp.zeros((HALF, 128), jnp.float32)
            put(0, ((one, zero),) * 3)
            lax.fori_loop(1, TOP + 1, step, tuple(base), unroll=4)

    q = q_ref[...]

    def eighths(v):
        return (v[0:8] + v[8:16]) + (v[16:24] + v[24:32])

    for j in range(SPLIT):

        def mode(i, carry, j=j):
            k = kc * CHUNK + j * PART + i
            at = k * 5
            h = idx_ref[at]
            cx, sx = rows_of(xc, h), rows_of(xs, h)
            cy, sy = rows_of(yc, idx_ref[at + 1]), rows_of(ys, idx_ref[at + 2])
            cz, sz = rows_of(zc, idx_ref[at + 3]), rows_of(zs, idx_ref[at + 4])
            cp = cx * cy - sx * sy
            sp = cx * sy + sx * cy
            c = cp * cz - sp * sz
            s = cp * sz + sp * cz
            e_refs[j][0, i, 0] = c
            e_refs[j][0, i, 1] = s
            acc[2 * k] += eighths(q * c)
            acc[2 * k + 1] += eighths(q * s)
            return carry

        lax.fori_loop(0, PART, mode, 0, unroll=8)

    @pl.when((b == pl.num_programs(0) - 1) & (kc == pl.num_programs(1) - 1))
    def _():
        rows = acc[:, 0, :]
        for r in range(1, 8):
            rows = rows + acc[:, r, :]
        ones = jnp.ones((8, 128), jnp.float32)
        s_ref[...] = lax.dot_general(
            ones,
            rows,
            (((1,), (1,)), ((), ())),
            precision=lax.Precision.HIGHEST,
            preferred_element_type=jnp.float32,
        )


def response_kernel(w_ref, *refs):
    e_refs = refs[:SPLIT]
    o_ref = refs[SPLIT]
    kc = pl.program_id(1)
    modes = (w_ref.shape[0] - 1) // 5

    @pl.when(kc == 0)
    def _():
        for t in range(2):
            o_ref[t, : 4 * HALF] = jnp.zeros((4 * HALF, 128), jnp.float32)
            o_ref[t, 4 * HALF :] = jnp.full((8, 128), w_ref[5 * modes], jnp.float32)

    def mine(c):
        part = slice(HALF * c, HALF * (c + 1))
        return jnp.concatenate([o_ref[0, part], o_ref[1, part]], axis=0)

    state = tuple(mine(c) for c in range(4))
    for j in range(SPLIT):

        def mode(i, carry, j=j):
            f0, f1, f2, p = carry
            at = (kc * CHUNK + j * PART + i) * 5
            wr, wi = w_ref[at], w_ref[at + 1]
            c = e_refs[j][0, i, 0]
            s = e_refs[j][0, i, 1]
            p = p + (wr * c + wi * s)
            g = wr * s - wi * c
            return (f0 + w_ref[at + 2] * g, f1 + w_ref[at + 3] * g, f2 + w_ref[at + 4] * g, p)

        state = lax.fori_loop(0, PART, mode, state, unroll=8)
    for c in range(4):
        o_ref[0, HALF * c : HALF * (c + 1)] = state[c][:HALF]
        o_ref[1, HALF * c : HALF * (c + 1)] = state[c][HALF:]


def on_device(scaled_coordinate_array, particle_charge_list, reciprocal_triples):
    local_atoms = scaled_coordinate_array.shape[1]
    modes = reciprocal_triples.shape[1]
    n_atom = lax.axis_size("atom")
    n_kvec = lax.axis_size("kvec")
    natoms = local_atoms * n_atom
    blocks = local_atoms // BLOCK
    chunks = modes // CHUNK

    triples = reciprocal_triples * jnp.where(reciprocal_triples[0:1] < 0, -1, 1)
    table = 2.0 * math.pi * triples.astype(jnp.float32)
    norm = jnp.sum(table * table, axis=0)
    damping = 4.0 * math.pi * jnp.exp(-norm / 1600000.0) / norm
    idx = ROWS * jnp.stack(
        [
            triples[0],
            jnp.abs(triples[1]),
            triples[1] + TOP,
            jnp.abs(triples[2]),
            triples[2] + TOP,
        ],
        axis=1,
    ).reshape(5 * modes)
    xyz = scaled_coordinate_array.reshape(3, local_atoms // 128, 128)
    q = particle_charge_list.reshape(local_atoms // 128, 128)

    e_spec = pl.BlockSpec((1, PART, 2, ROWS, 128), lambda b, c: (b, c, 0, 0, 0))
    e_shape = jax.ShapeDtypeStruct((blocks, modes // SPLIT, 2, ROWS, 128), jnp.float32)
    *e, s = pl.pallas_call(
        phases_kernel,
        grid=(blocks, chunks),
        in_specs=[
            pl.BlockSpec(memory_space=pltpu.SMEM),
            pl.BlockSpec((3, ROWS, 128), lambda b, c: (0, b, 0)),
            pl.BlockSpec((ROWS, 128), lambda b, c: (b, 0)),
        ],
        out_specs=[e_spec] * SPLIT + [pl.BlockSpec((8, 2 * modes), lambda b, c: (0, 0))],
        out_shape=[e_shape] * SPLIT + [jax.ShapeDtypeStruct((8, 2 * modes), jnp.float32)],
        scratch_shapes=[
            pltpu.VMEM(((TOP + 1) * ROWS, 128), jnp.float32),
            pltpu.VMEM(((TOP + 1) * ROWS, 128), jnp.float32),
            pltpu.VMEM(((TOP + 1) * ROWS, 128), jnp.float32),
            pltpu.VMEM(((2 * TOP + 1) * ROWS, 128), jnp.float32),
            pltpu.VMEM(((TOP + 1) * ROWS, 128), jnp.float32),
            pltpu.VMEM(((2 * TOP + 1) * ROWS, 128), jnp.float32),
            pltpu.VMEM((2 * modes, 8, 128), jnp.float32),
        ],
        compiler_params=pltpu.CompilerParams(
            dimension_semantics=("arbitrary", "arbitrary"), vmem_limit_bytes=48 * MIB
        ),
    )(idx, xyz, q)

    share = jnp.broadcast_to(s[0:1], (n_atom, 2 * modes))
    total = lax.all_to_all(share, "atom", 0, 0, tiled=True).sum(axis=0)
    total = total.reshape(modes, 2)
    cosine, sine = total[:, 0], total[:, 1]
    partial_energy = 50.0 / natoms * jnp.sum(damping * (cosine * cosine + sine * sine))
    w = jnp.concatenate([(damping * cosine)[None], (damping * sine)[None], table])
    w = jnp.concatenate([w.T.reshape(5 * modes), partial_energy.reshape(1)])

    terms = pl.pallas_call(
        response_kernel,
        grid=(blocks, chunks),
        in_specs=[pl.BlockSpec(memory_space=pltpu.SMEM)] + [e_spec] * SPLIT,
        out_specs=pl.BlockSpec((2, 4 * HALF + 8, 128), lambda b, c: (b, 0, 0)),
        out_shape=jax.ShapeDtypeStruct((n_kvec, 4 * HALF + 8, 128), jnp.float32),
        compiler_params=pltpu.CompilerParams(
            dimension_semantics=("arbitrary", "arbitrary"), vmem_limit_bytes=48 * MIB
        ),
    )(w, *e)

    own = lax.all_to_all(terms, "kvec", 0, 0, tiled=True).sum(axis=0)
    energy = own[4 * HALF, 0]
    copies = jnp.broadcast_to(own[None, : 4 * HALF], (n_kvec, 4 * HALF, 128))
    summed = lax.all_to_all(copies, "kvec", 0, 0, tiled=True)
    summed = summed.reshape(n_kvec, 4, HALF * 128).transpose(1, 0, 2).reshape(4, local_atoms)
    scale = 1.0 / math.sqrt(natoms)
    forces = summed[:3] * particle_charge_list[None, :] * scale
    potential = summed[3] * (400.0 * scale)
    return (forces, potential, energy)


def solution(mesh):
    return jax.shard_map(
        on_device,
        mesh=mesh,
        in_specs=(P(None, "atom"), P("atom"), P(None, "kvec")),
        out_specs=(P(None, "atom"), P("atom"), P()),
        check_vma=False,
    )
```

```python
import math

import jax
import jax.numpy as jnp
from jax import lax
from jax.experimental import pallas as pl
from jax.experimental.pallas import tpu as pltpu
from jax.sharding import PartitionSpec as P

TOP = 128
STRIDE = 16
BLOCK = 4096
ROWS = BLOCK // 128
HALF = ROWS // 2
PART = 32
SLOTS = 8
UNROLL = 8
MIB = 1 << 20


def rows_of(ref, start):
    return ref[pl.ds(pl.multiple_of(start, ROWS), ROWS), :]


def times(a, b):
    return a[0] * b[0] - a[1] * b[1], a[0] * b[1] + a[1] * b[0]


def turn(x):
    y = 4.0 * (x - jnp.round(x))
    n = jnp.round(y)
    r = (0.5 * math.pi) * (y - n)
    z = r * r
    s = r + r * z * (-1.6666654611e-1 + z * (8.3321608736e-3 - 1.9515295891e-4 * z))
    c = 4.166664568298827e-2 + z * (-1.388731625493765e-3 + 2.443315711809948e-5 * z)
    c = 1.0 + z * (c * z - 0.5)
    odd = jnp.abs(n) == 1.0
    cos = jnp.where(odd, s, c)
    sin = jnp.where(odd, c, s)
    cos = jnp.where((n > 0.5) | (n < -1.5), -cos, cos)
    sin = jnp.where((n > 1.5) | (n < -0.5), -sin, sin)
    return cos, sin


def fill_powers(x, low, cos_ref, sin_ref, signed):
    small = [(jnp.ones_like(x), jnp.zeros_like(x)), turn(x)]
    for b in range(2, STRIDE // 2 + 1):
        small.append(times(small[b // 2], small[b - b // 2]))
    big = times(small[-1], small[-1])

    def put(h, c, s):
        def at(r):
            return pl.ds(pl.multiple_of(r * ROWS + low, 8), HALF)

        cos_ref[at(h)] = c
        if signed:
            sin_ref[at(TOP + h)] = s
            sin_ref[at(TOP - h)] = -s
        else:
            sin_ref[at(h)] = s

    for b in range(STRIDE // 2):
        put(b, *small[b])

    def around(a, state, both):
        c, s = state
        put(STRIDE * a, c, s)
        for b in range(1, STRIDE // 2 + 1):
            cb, sb = small[b]
            cc, ss, sc, cs = c * cb, s * sb, s * cb, c * sb
            put(STRIDE * a - b, cc + ss, sc - cs)
            if both and b < STRIDE // 2:
                put(STRIDE * a + b, cc - ss, sc + cs)

    def step(a, state):
        around(a, state, True)
        return times(state, big)

    last = lax.fori_loop(1, TOP // STRIDE, step, big)
    around(TOP // STRIDE, last, False)


def eighths(v):
    return (v[0:8] + v[8:16]) + (v[16:24] + v[24:32])


def phases_kernel(idx_ref, xyz_ref, q_ref, e_ref, s_ref, xc, xs, yc, ys, zc, zs, acc, ring, sems):
    blocks, modes = e_ref.shape[0], e_ref.shape[1]
    parts = modes // PART

    def clear(i, carry):
        acc[i] = jnp.zeros((8, 128), jnp.float32)
        return carry

    lax.fori_loop(0, acc.shape[0], clear, 0, unroll=8)

    def copy(slot, b, p):
        return pltpu.make_async_copy(
            ring.at[slot], e_ref.at[b, pl.ds(p * PART, PART)], sems.at[slot]
        )

    def block(b, carry):
        for low in (0, HALF):
            for d, (c_ref, s_ref_) in enumerate(((xc, xs), (yc, ys), (zc, zs))):
                x = xyz_ref[d, pl.ds(pl.multiple_of(b * ROWS + low, HALF), HALF)]
                fill_powers(x, low, c_ref, s_ref_, d > 0)
        q = q_ref[pl.ds(pl.multiple_of(b * ROWS, ROWS), ROWS)]

        def part(p, carry):
            t = b * parts + p
            slot = lax.rem(t, SLOTS)

            @pl.when(t >= SLOTS)
            def _():
                copy(slot, b, p).wait()

            def mode(i, carry):
                k = p * PART + i
                at = k * 5
                h = idx_ref[at]
                first = rows_of(xc, h), rows_of(xs, h)
                second = rows_of(yc, idx_ref[at + 1]), rows_of(ys, idx_ref[at + 2])
                third = rows_of(zc, idx_ref[at + 3]), rows_of(zs, idx_ref[at + 4])
                c, s = times(times(first, second), third)
                ring[slot, i, 0] = c
                ring[slot, i, 1] = s
                acc[2 * k] += eighths(q * c)
                acc[2 * k + 1] += eighths(q * s)
                return carry

            lax.fori_loop(0, PART, mode, 0, unroll=UNROLL)
            copy(slot, b, p).start()
            return carry

        return lax.fori_loop(0, parts, part, carry)

    lax.fori_loop(0, blocks, block, 0)

    for at in range(0, 2 * modes, 128):
        rows = acc[at : at + 128, 0, :]
        for r in range(1, 8):
            rows = rows + acc[at : at + 128, r, :]
        line = jnp.sum(rows.T, axis=0, keepdims=True)
        s_ref[:, at : at + 128] = jnp.broadcast_to(line, (s_ref.shape[0], 128))

    def drain(slot, carry):
        copy(slot, 0, 0).wait()
        return carry

    lax.fori_loop(0, SLOTS, drain, 0)


def response_kernel(w_ref, e_ref, o_ref, ring, sems):
    blocks, modes = e_ref.shape[0], e_ref.shape[1]
    parts = modes // PART

    def copy(slot, b, p):
        return pltpu.make_async_copy(
            e_ref.at[b, pl.ds(p * PART, PART)], ring.at[slot], sems.at[slot]
        )

    def fetch(t):
        copy(lax.rem(t, SLOTS), t // parts, lax.rem(t, parts)).start()

    def first(t, carry):
        fetch(t)
        return carry

    lax.fori_loop(0, SLOTS, first, 0)
    zero = jnp.zeros((ROWS, 128), jnp.float32)

    def block(b, carry):
        def part(p, state):
            t = b * parts + p
            slot = lax.rem(t, SLOTS)
            copy(slot, b, p).wait()

            def mode(i, state):
                f0, f1, f2, pot = state
                at = (p * PART + i) * 5
                wr, wi = w_ref[at], w_ref[at + 1]
                c = ring[slot, i, 0]
                s = ring[slot, i, 1]
                pot = pot + (wr * c + wi * s)
                g = wr * s - wi * c
                return (
                    f0 + w_ref[at + 2] * g,
                    f1 + w_ref[at + 3] * g,
                    f2 + w_ref[at + 4] * g,
                    pot,
                )

            state = lax.fori_loop(0, PART, mode, state, unroll=UNROLL)

            @pl.when(t + SLOTS < blocks * parts)
            def _():
                fetch(t + SLOTS)

            return state

        state = lax.fori_loop(0, parts, part, (zero,) * 4)
        for t in range(2):
            for c in range(4):
                o_ref[2 * b + t, HALF * c : HALF * (c + 1)] = state[c][HALF * t : HALF * (t + 1)]
            o_ref[2 * b + t, 4 * HALF :] = jnp.full((8, 128), w_ref[5 * modes], jnp.float32)
        return carry

    lax.fori_loop(0, blocks, block, 0)


def on_device(scaled_coordinate_array, particle_charge_list, reciprocal_triples):
    local_atoms = scaled_coordinate_array.shape[1]
    modes = reciprocal_triples.shape[1]
    n_atom = lax.axis_size("atom")
    n_kvec = lax.axis_size("kvec")
    natoms = local_atoms * n_atom
    blocks = local_atoms // BLOCK

    triples = reciprocal_triples * jnp.where(reciprocal_triples[0:1] < 0, -1, 1)
    table = 2.0 * math.pi * triples.astype(jnp.float32)
    norm = jnp.sum(table * table, axis=0)
    damping = 4.0 * math.pi * jnp.exp(-norm / 1600000.0) / norm
    idx = ROWS * jnp.stack(
        [
            triples[0],
            jnp.abs(triples[1]),
            triples[1] + TOP,
            jnp.abs(triples[2]),
            triples[2] + TOP,
        ],
        axis=1,
    ).reshape(5 * modes)
    xyz = scaled_coordinate_array.reshape(3, local_atoms // 128, 128)
    q = particle_charge_list.reshape(local_atoms // 128, 128)

    smem = pl.BlockSpec(memory_space=pltpu.SMEM)
    vmem = pl.BlockSpec(memory_space=pltpu.VMEM)
    hbm = pl.BlockSpec(memory_space=pl.ANY)
    ring = [
        pltpu.VMEM((SLOTS, PART, 2, ROWS, 128), jnp.float32),
        pltpu.SemaphoreType.DMA((SLOTS,)),
    ]
    positive = pltpu.VMEM(((TOP + 1) * ROWS, 128), jnp.float32)
    both = pltpu.VMEM(((2 * TOP + 1) * ROWS, 128), jnp.float32)
    e, share = pl.pallas_call(
        phases_kernel,
        in_specs=[smem, vmem, vmem],
        out_specs=[hbm, vmem],
        out_shape=[
            jax.ShapeDtypeStruct((blocks, modes, 2, ROWS, 128), jnp.float32),
            jax.ShapeDtypeStruct((n_atom, 2 * modes), jnp.float32),
        ],
        scratch_shapes=[
            positive,
            positive,
            positive,
            both,
            positive,
            both,
            pltpu.VMEM((2 * modes, 8, 128), jnp.float32),
        ]
        + ring,
        compiler_params=pltpu.CompilerParams(vmem_limit_bytes=48 * MIB),
    )(idx, xyz, q)

    total = lax.all_to_all(share, "atom", 0, 0, tiled=True).sum(axis=0)
    total = total.reshape(modes, 2)
    cosine, sine = total[:, 0], total[:, 1]
    partial_energy = 50.0 / natoms * jnp.sum(damping * (cosine * cosine + sine * sine))
    w = jnp.concatenate([(damping * cosine)[None], (damping * sine)[None], table])
    w = jnp.concatenate([w.T.reshape(5 * modes), partial_energy.reshape(1)])

    terms = pl.pallas_call(
        response_kernel,
        in_specs=[smem, hbm],
        out_specs=vmem,
        out_shape=jax.ShapeDtypeStruct((n_kvec, 4 * HALF + 8, 128), jnp.float32),
        scratch_shapes=ring,
        compiler_params=pltpu.CompilerParams(vmem_limit_bytes=24 * MIB),
    )(w, e)

    own = lax.all_to_all(terms, "kvec", 0, 0, tiled=True).sum(axis=0)
    energy = own[4 * HALF, 0]
    copies = jnp.broadcast_to(own[None, : 4 * HALF], (n_kvec, 4 * HALF, 128))
    summed = lax.all_to_all(copies, "kvec", 0, 0, tiled=True)
    summed = summed.reshape(n_kvec, 4, HALF * 128).transpose(1, 0, 2).reshape(4, local_atoms)
    scale = 1.0 / math.sqrt(natoms)
    forces = summed[:3] * particle_charge_list[None, :] * scale
    potential = summed[3] * (400.0 * scale)
    return (forces, potential, energy)


def solution(mesh):
    return jax.shard_map(
        on_device,
        mesh=mesh,
        in_specs=(P(None, "atom"), P("atom"), P(None, "kvec")),
        out_specs=(P(None, "atom"), P("atom"), P()),
        check_vma=False,
    )
```

```python
import functools
import math

import jax
import jax.numpy as jnp
from jax import lax
from jax.experimental import pallas as pl
from jax.experimental.pallas import tpu as pltpu
from jax.sharding import PartitionSpec as P

TOP = 128
STRIDE = 16
BLOCK = 4096
ROWS = BLOCK // 128
HALF = ROWS // 2
PART = 32
SLOTS = 8
UNROLL = 16
TINY = 1e-6
KINDS = 8
MIB = 1 << 20


def rows_of(ref, start):
    return ref[pl.ds(pl.multiple_of(start, ROWS), ROWS), :]


def times(a, b):
    return a[0] * b[0] - a[1] * b[1], a[0] * b[1] + a[1] * b[0]


def turn(x):
    y = 4.0 * (x - jnp.round(x))
    n = jnp.round(y)
    r = (0.5 * math.pi) * (y - n)
    z = r * r
    s = r + r * z * (-1.6666654611e-1 + z * (8.3321608736e-3 - 1.9515295891e-4 * z))
    c = 4.166664568298827e-2 + z * (-1.388731625493765e-3 + 2.443315711809948e-5 * z)
    c = 1.0 + z * (c * z - 0.5)
    odd = jnp.abs(n) == 1.0
    cos = jnp.where(odd, s, c)
    sin = jnp.where(odd, c, s)
    cos = jnp.where((n > 0.5) | (n < -1.5), -cos, cos)
    sin = jnp.where((n > 1.5) | (n < -0.5), -sin, sin)
    return cos, sin


def fill_powers(x, weight, low, cos_ref, sin_ref, signed):
    small = [(jnp.ones_like(x), jnp.zeros_like(x)), turn(x)]
    for b in range(2, STRIDE // 2 + 1):
        small.append(times(small[b // 2], small[b - b // 2]))
    big = times(small[-1], small[-1])

    def put(h, c, s):
        def at(r):
            return pl.ds(pl.multiple_of(r * ROWS + low, 8), HALF)

        cos_ref[at(h)] = c
        if signed:
            sin_ref[at(TOP + h)] = s
            sin_ref[at(TOP - h)] = -s
        else:
            sin_ref[at(h)] = s

    def weighted(v):
        return v if weight is None else (weight * v[0], weight * v[1])

    for b in range(STRIDE // 2):
        put(b, *weighted(small[b]))

    def around(a, state, both):
        c, s = state
        put(STRIDE * a, c, s)
        for b in range(1, STRIDE // 2 + 1):
            cb, sb = small[b]
            cc, ss, sc, cs = c * cb, s * sb, s * cb, c * sb
            put(STRIDE * a - b, cc + ss, sc - cs)
            if both and b < STRIDE // 2:
                put(STRIDE * a + b, cc - ss, sc + cs)

    def step(a, state):
        around(a, state, True)
        return times(state, big)

    last = lax.fori_loop(1, TOP // STRIDE, step, weighted(big))
    around(TOP // STRIDE, last, False)


def eighths(v):
    return (v[0:8] + v[8:16]) + (v[16:24] + v[24:32])


def nonzero(q):
    return jnp.where(jnp.abs(q) < TINY, TINY, q)


def lines(v):
    return [v[:, at : at + 128] for at in range(0, v.shape[1], 128)]


def half_space(triples):
    return jnp.where(triples[0:1] < 0, -triples, triples)


def phases_kernel(
    trip_ref, x_ref, q_ref, e_ref, s_ref,
    xc, xs, yc, ys, zc, zs, acc, xyz, stage, idx, idx_sem, ring, sems,
):
    blocks, modes = e_ref.shape[0], e_ref.shape[1]
    parts = modes // PART
    triples = half_space(trip_ref[...])
    h, k, l = triples[0:1], triples[1:2], triples[2:3]
    for kind, row in enumerate((h, jnp.abs(k), k + TOP, jnp.abs(l), l + TOP)):
        for r, line in enumerate(lines(ROWS * row)):
            stage[r, kind : kind + 1] = line
    for kind in range(5, KINDS):
        for r in range(modes // 128):
            stage[r, kind : kind + 1] = jnp.zeros((1, 128), jnp.int32)
    to_scalars = pltpu.make_async_copy(stage, idx, idx_sem)
    to_scalars.start()

    def clear(i, carry):
        acc[i] = jnp.zeros((8, 128), jnp.float32)
        return carry

    lax.fori_loop(0, acc.shape[0], clear, 0, unroll=8)

    def fold(i, carry):
        for d in range(3):
            xyz[d, pl.ds(i, 1)] = x_ref[d : d + 1, pl.ds(pl.multiple_of(i * 128, 128), 128)]
        return carry

    lax.fori_loop(0, xyz.shape[1], fold, 0, unroll=16)
    faint = jnp.max(jnp.where(jnp.abs(q_ref[...]) < TINY, 1.0, 0.0)) > 0.0

    def copy(slot, b, p):
        return pltpu.make_async_copy(
            ring.at[slot], e_ref.at[b, pl.ds(p * PART, PART)], sems.at[slot]
        )

    def block(b, carry):
        for low in (0, HALF):
            here = pl.ds(pl.multiple_of(b * ROWS + low, HALF), HALF)
            for d, (c_ref, s_ref_) in enumerate(((xc, xs), (yc, ys), (zc, zs))):
                weight = nonzero(q_ref[here]) if d == 2 else None
                fill_powers(xyz[d, here], weight, low, c_ref, s_ref_, d > 0)

        @pl.when(b == 0)
        def _():
            to_scalars.wait()

        def part(p, carry):
            t = b * parts + p
            slot = lax.rem(t, SLOTS)
            r = (p * PART) // 128
            lane = lax.rem(p * PART, 128)

            @pl.when(t >= SLOTS)
            def _():
                copy(slot, b, p).wait()

            def mode(i, ratio):
                at = lane + i
                first = rows_of(xc, idx[r, 0, at]), rows_of(xs, idx[r, 0, at])
                second = rows_of(yc, idx[r, 1, at]), rows_of(ys, idx[r, 2, at])
                third = rows_of(zc, idx[r, 3, at]), rows_of(zs, idx[r, 4, at])
                c, s = times(times(first, second), third)
                ring[slot, i, 0] = c
                ring[slot, i, 1] = s
                if ratio is not None:
                    c, s = ratio * c, ratio * s
                acc[p * PART + i] += eighths(c)
                acc[modes + p * PART + i] += eighths(s)

            @pl.when(faint)
            def _():
                q = q_ref[pl.ds(pl.multiple_of(b * ROWS, ROWS), ROWS)]
                ratio = q / nonzero(q)
                lax.fori_loop(0, PART, lambda i, c: (mode(i, ratio), c)[1], 0)

            @pl.when(jnp.logical_not(faint))
            def _():
                lax.fori_loop(0, PART, lambda i, c: (mode(i, None), c)[1], 0, unroll=UNROLL)

            copy(slot, b, p).start()
            return carry

        return lax.fori_loop(0, parts, part, carry)

    lax.fori_loop(0, blocks, block, 0)

    for r in range(8):
        rows = acc[128 * r : 128 * (r + 1), 0, :]
        for sub in range(1, 8):
            rows = rows + acc[128 * r : 128 * (r + 1), sub, :]
        s_ref[r : r + 1] = jnp.sum(rows.T, axis=0, keepdims=True)

    def drain(slot, carry):
        copy(slot, 0, 0).wait()
        return carry

    lax.fori_loop(0, SLOTS, drain, 0)


def response_kernel(scale, got_ref, trip_ref, e_ref, o_ref, stage, w, w_sem, ring, sems):
    blocks, modes = e_ref.shape[0], e_ref.shape[1]
    parts = modes // PART
    n_lines = modes // 128

    def copy(slot, b, p):
        return pltpu.make_async_copy(
            e_ref.at[b, pl.ds(p * PART, PART)], ring.at[slot], sems.at[slot]
        )

    def fetch(t):
        copy(lax.rem(t, SLOTS), t // parts, lax.rem(t, parts)).start()

    def first(t, carry):
        fetch(t)
        return carry

    lax.fori_loop(0, SLOTS, first, 0)

    total = got_ref[0]
    for i in range(1, got_ref.shape[0]):
        total = total + got_ref[i]
    cosine, sine = total[:n_lines], total[n_lines:]
    triples = half_space(trip_ref[...])
    table = [
        (2.0 * math.pi) * jnp.concatenate(lines(triples[d : d + 1]), axis=0).astype(jnp.float32)
        for d in range(3)
    ]
    norm = table[0] * table[0] + table[1] * table[1] + table[2] * table[2]
    damping = 4.0 * math.pi * jnp.exp(-norm / 1600000.0) / norm
    energy = scale * jnp.sum(damping * (cosine * cosine + sine * sine))
    for kind, rows in enumerate([damping * cosine, damping * sine] + table):
        for r in range(n_lines):
            stage[r, kind : kind + 1] = rows[r : r + 1]
    for kind in range(5, KINDS):
        for r in range(n_lines):
            stage[r, kind : kind + 1] = jnp.zeros((1, 128), jnp.float32)
    to_scalars = pltpu.make_async_copy(stage, w, w_sem)
    to_scalars.start()
    to_scalars.wait()
    zero = jnp.zeros((ROWS, 128), jnp.float32)

    def block(b, carry):
        def part(p, state):
            t = b * parts + p
            slot = lax.rem(t, SLOTS)
            r = (p * PART) // 128
            lane = lax.rem(p * PART, 128)
            copy(slot, b, p).wait()

            def mode(i, state):
                f0, f1, f2, pot = state
                at = lane + i
                wr, wi = w[r, 0, at], w[r, 1, at]
                c = ring[slot, i, 0]
                s = ring[slot, i, 1]
                pot = pot + (wr * c + wi * s)
                g = wr * s - wi * c
                return f0 + w[r, 2, at] * g, f1 + w[r, 3, at] * g, f2 + w[r, 4, at] * g, pot

            state = lax.fori_loop(0, PART, mode, state, unroll=UNROLL)

            @pl.when(t + SLOTS < blocks * parts)
            def _():
                fetch(t + SLOTS)

            return state

        state = lax.fori_loop(0, parts, part, (zero,) * 4)
        for t in range(2):
            for c in range(4):
                o_ref[2 * b + t, HALF * c : HALF * (c + 1)] = state[c][HALF * t : HALF * (t + 1)]
            o_ref[2 * b + t, 4 * HALF :] = jnp.full((8, 128), energy, jnp.float32)
        return carry

    lax.fori_loop(0, blocks, block, 0)


def on_device(scaled_coordinate_array, particle_charge_list, reciprocal_triples):
    local_atoms = scaled_coordinate_array.shape[1]
    modes = reciprocal_triples.shape[1]
    n_atom = lax.axis_size("atom")
    n_kvec = lax.axis_size("kvec")
    natoms = local_atoms * n_atom
    blocks = local_atoms // BLOCK
    n_lines = modes // 128
    q = particle_charge_list.reshape(local_atoms // 128, 128)

    vmem = pl.BlockSpec(memory_space=pltpu.VMEM)
    hbm = pl.BlockSpec(memory_space=pl.ANY)
    ring = [
        pltpu.VMEM((SLOTS, PART, 2, ROWS, 128), jnp.float32),
        pltpu.SemaphoreType.DMA((SLOTS,)),
    ]

    def scalars(dtype):
        return [
            pltpu.VMEM((n_lines, KINDS, 128), dtype),
            pltpu.SMEM((n_lines, KINDS, 128), dtype),
            pltpu.SemaphoreType.DMA(()),
        ]

    positive = pltpu.VMEM(((TOP + 1) * ROWS, 128), jnp.float32)
    both = pltpu.VMEM(((2 * TOP + 1) * ROWS, 128), jnp.float32)
    e, share = pl.pallas_call(
        phases_kernel,
        in_specs=[vmem, vmem, vmem],
        out_specs=[hbm, vmem],
        out_shape=[
            jax.ShapeDtypeStruct((blocks, modes, 2, ROWS, 128), jnp.float32),
            jax.ShapeDtypeStruct((8, 128), jnp.float32),
        ],
        scratch_shapes=[
            positive,
            positive,
            positive,
            both,
            positive,
            both,
            pltpu.VMEM((2 * modes, 8, 128), jnp.float32),
            pltpu.VMEM((3, local_atoms // 128, 128), jnp.float32),
        ]
        + scalars(jnp.int32)
        + ring,
        compiler_params=pltpu.CompilerParams(vmem_limit_bytes=48 * MIB),
    )(reciprocal_triples, scaled_coordinate_array, q)

    share = share + lax.ppermute(share, "atom", [(i, i ^ 1) for i in range(n_atom)])
    share = jnp.broadcast_to(share[None], (n_atom // 2, 8, 128))
    cores = [[c + 2 * m for m in range(n_atom // 2)] for c in range(2)]
    got = lax.all_to_all(share, "atom", 0, 0, tiled=True, axis_index_groups=cores)

    terms = pl.pallas_call(
        functools.partial(response_kernel, 50.0 / natoms),
        in_specs=[vmem, vmem, hbm],
        out_specs=vmem,
        out_shape=jax.ShapeDtypeStruct((n_kvec, 4 * HALF + 8, 128), jnp.float32),
        scratch_shapes=scalars(jnp.float32) + ring,
        compiler_params=pltpu.CompilerParams(vmem_limit_bytes=24 * MIB),
    )(got, reciprocal_triples, e)

    own = lax.all_to_all(terms, "kvec", 0, 0, tiled=True).sum(axis=0)
    energy = own[4 * HALF, 0]
    copies = jnp.broadcast_to(own[None, : 4 * HALF], (n_kvec, 4 * HALF, 128))
    summed = lax.all_to_all(copies, "kvec", 0, 0, tiled=True)
    summed = summed.reshape(n_kvec, 4, HALF * 128).transpose(1, 0, 2).reshape(4, local_atoms)
    scale = 1.0 / math.sqrt(natoms)
    forces = summed[:3] * scale
    potential = summed[3] * (400.0 * scale) / nonzero(particle_charge_list)
    return (forces, potential, energy)


def solution(mesh):
    return jax.shard_map(
        on_device,
        mesh=mesh,
        in_specs=(P(None, "atom"), P("atom"), P(None, "kvec")),
        out_specs=(P(None, "atom"), P("atom"), P()),
        check_vma=False,
    )
```

```python
import functools
import math

import jax
import jax.numpy as jnp
from jax import lax
from jax.experimental import pallas as pl
from jax.experimental.pallas import tpu as pltpu
from jax.sharding import PartitionSpec as P

TOP = 128
STRIDE = 16
BLOCK = 4096
ROWS = BLOCK // 128
HALF = ROWS // 2
PART = 32
SLOTS = 8
WRITE_PART = 64
WRITE_SLOTS = 5
UNROLL = 16
GROUP = 8
TINY = 1e-6
KINDS = 5
MIB = 1 << 20


def rows_of(ref, start):
    return ref[pl.ds(pl.multiple_of(start, ROWS), ROWS), :]


def times(a, b):
    return a[0] * b[0] - a[1] * b[1], a[0] * b[1] + a[1] * b[0]


def turn(x):
    y = 4.0 * (x - jnp.round(x))
    n = jnp.round(y)
    r = (0.5 * math.pi) * (y - n)
    z = r * r
    s = r + r * z * (-1.6666654611e-1 + z * (8.3321608736e-3 - 1.9515295891e-4 * z))
    c = 4.166664568298827e-2 + z * (-1.388731625493765e-3 + 2.443315711809948e-5 * z)
    c = 1.0 + z * (c * z - 0.5)
    odd = jnp.abs(n) == 1.0
    cos = jnp.where(odd, s, c)
    sin = jnp.where(odd, c, s)
    cos = jnp.where((n > 0.5) | (n < -1.5), -cos, cos)
    sin = jnp.where((n > 1.5) | (n < -0.5), -sin, sin)
    return cos, sin


def fill_powers(x, weight, low, cos_ref, sin_ref, signed):
    small = [(jnp.ones_like(x), jnp.zeros_like(x)), turn(x)]
    for b in range(2, STRIDE // 2 + 1):
        small.append(times(small[b // 2], small[b - b // 2]))
    big = times(small[-1], small[-1])

    def put(h, c, s):
        def at(r):
            return pl.ds(pl.multiple_of(r * ROWS + low, 8), HALF)

        cos_ref[at(h)] = c
        if signed:
            sin_ref[at(TOP + h)] = s
            sin_ref[at(TOP - h)] = -s
        else:
            sin_ref[at(h)] = s

    def weighted(v):
        return v if weight is None else (weight * v[0], weight * v[1])

    for b in range(STRIDE // 2):
        put(b, *weighted(small[b]))

    def around(a, state, both):
        c, s = state
        put(STRIDE * a, c, s)
        for b in range(1, STRIDE // 2 + 1):
            cb, sb = small[b]
            cc, ss, sc, cs = c * cb, s * sb, s * cb, c * sb
            put(STRIDE * a - b, cc + ss, sc - cs)
            if both and b < STRIDE // 2:
                put(STRIDE * a + b, cc - ss, sc + cs)

    def step(a, state):
        around(a, state, True)
        return times(state, big)

    last = lax.fori_loop(1, TOP // STRIDE, step, weighted(big), unroll=TOP // STRIDE - 1)
    around(TOP // STRIDE, last, False)


def eighths(v):
    return (v[0:8] + v[8:16]) + (v[16:24] + v[24:32])


def nonzero(q):
    return jnp.where(jnp.abs(q) < TINY, TINY, q)


def lines(v):
    return [v[:, at : at + 128] for at in range(0, v.shape[1], 128)]


def to_scalars(stage, scalars, sems):
    return [
        pltpu.make_async_copy(stage.at[i], scalars.at[pl.ds(128 * i, 128)], sems.at[i])
        for i in range(stage.shape[0])
    ]


def half_space(triples):
    return jnp.where(triples[0:1] < 0, -triples, triples)


def phases_kernel(
    trip_hbm, x_hbm, q_hbm, e_ref, s_ref,
    xc, xs, yc, ys, zc, zs, acc_c, acc_s, trip_ref, x_ref, q_ref, in_sems,
    xyz, stage, idx, idx_sem, ring, sems,
):
    blocks, modes = e_ref.shape[0], e_ref.shape[1]
    parts = modes // WRITE_PART
    loads = [
        pltpu.make_async_copy(src, dst, in_sems.at[i])
        for i, (src, dst) in enumerate(((x_hbm, x_ref), (q_hbm, q_ref), (trip_hbm, trip_ref)))
    ]
    for load in loads:
        load.start()

    def clear(i, carry):
        at = pl.ds(pl.multiple_of(i * 128, 128), 128)
        acc_c[at] = jnp.zeros((128, 128), jnp.float32)
        acc_s[at] = jnp.zeros((128, 128), jnp.float32)
        return carry

    lax.fori_loop(0, acc_c.shape[0] // 128, clear, 0)
    for load in loads:
        load.wait()
    triples = half_space(trip_ref[...])
    h, k, l = triples[0:1], triples[1:2], triples[2:3]
    for kind, row in enumerate((h, jnp.abs(k), k + TOP, jnp.abs(l), l + TOP)):
        for r, line in enumerate(lines(ROWS * row)):
            at = kind * (modes // 128) + r
            stage[at : at + 1] = line
    for move in to_scalars(stage, idx, idx_sem):
        move.start()

    def fold(i, carry):
        for d in range(3):
            xyz[d, pl.ds(i, 1)] = x_ref[d : d + 1, pl.ds(pl.multiple_of(i * 128, 128), 128)]
        return carry

    lax.fori_loop(0, xyz.shape[1], fold, 0, unroll=16)
    faint = jnp.max(jnp.where(jnp.abs(q_ref[...]) < TINY, 1.0, 0.0)) > 0.0

    def copy(slot, b, p):
        return pltpu.make_async_copy(
            ring.at[slot], e_ref.at[b, pl.ds(p * WRITE_PART, WRITE_PART)], sems.at[slot]
        )

    def block(b, carry):
        for low in (0, HALF):
            here = pl.ds(pl.multiple_of(b * ROWS + low, HALF), HALF)
            for d, (c_ref, s_ref_) in enumerate(((xc, xs), (yc, ys), (zc, zs))):
                weight = nonzero(q_ref[here]) if d == 2 else None
                fill_powers(xyz[d, here], weight, low, c_ref, s_ref_, d > 0)

        @pl.when(b == 0)
        def _():
            for move in to_scalars(stage, idx, idx_sem):
                move.wait()

        def part(p, carry):
            t = b * parts + p
            slot = lax.rem(t, WRITE_SLOTS)

            @pl.when(t >= WRITE_SLOTS)
            def _():
                copy(slot, b, p).wait()

            def group(g, ratio):
                sums_c, sums_s = [], []
                for j in range(GROUP):
                    i = g * GROUP + j
                    k = p * WRITE_PART + i
                    h = idx[k]
                    first = rows_of(xc, h), rows_of(xs, h)
                    second = rows_of(yc, idx[modes + k]), rows_of(ys, idx[2 * modes + k])
                    third = rows_of(zc, idx[3 * modes + k]), rows_of(zs, idx[4 * modes + k])
                    c, s = times(times(first, second), third)
                    ring[slot, i, 0] = c
                    ring[slot, i, 1] = s
                    if ratio is not None:
                        c, s = ratio * c, ratio * s
                    sums_c.append(eighths(c))
                    sums_s.append(eighths(s))
                at = pl.ds(pl.multiple_of((p * WRITE_PART + g * GROUP) * 8, 8 * GROUP), 8 * GROUP)
                sums_c = acc_c[at] + jnp.concatenate(sums_c, axis=0)
                sums_s = acc_s[at] + jnp.concatenate(sums_s, axis=0)
                acc_c[at] = sums_c
                acc_s[at] = sums_s

            groups = WRITE_PART // GROUP

            @pl.when(faint)
            def _():
                q = q_ref[pl.ds(pl.multiple_of(b * ROWS, ROWS), ROWS)]
                ratio = q / nonzero(q)
                lax.fori_loop(0, groups, lambda g, c: (group(g, ratio), c)[1], 0)

            @pl.when(jnp.logical_not(faint))
            def _():
                lax.fori_loop(0, groups, lambda g, c: (group(g, None), c)[1], 0, unroll=UNROLL // GROUP)

            copy(slot, b, p).start()
            return carry

        return lax.fori_loop(0, parts, part, carry)

    lax.fori_loop(0, blocks, block, 0)

    for half, acc in enumerate((acc_c, acc_s)):
        for r in range(modes // 128):
            rows = acc[pl.ds(1024 * r, 128, stride=8)]
            for sub in range(1, 8):
                rows = rows + acc[pl.ds(1024 * r + sub, 128, stride=8)]
            at = half * (modes // 128) + r
            s_ref[at : at + 1] = jnp.sum(rows.T, axis=0, keepdims=True)

    def drain(slot, carry):
        copy(slot, 0, 0).wait()
        return carry

    lax.fori_loop(0, WRITE_SLOTS, drain, 0)


def response_kernel(scale, got_ref, trip_ref, e_ref, o_ref, stage, w, w_sem, ring, sems):
    blocks, modes = e_ref.shape[0], e_ref.shape[1]
    parts = modes // PART
    n_lines = modes // 128

    def copy(slot, b, p):
        return pltpu.make_async_copy(
            e_ref.at[b, pl.ds(p * PART, PART)], ring.at[slot], sems.at[slot]
        )

    def fetch(t):
        copy(lax.rem(t, SLOTS), t // parts, lax.rem(t, parts)).start()

    def first(t, carry):
        fetch(t)
        return carry

    lax.fori_loop(0, SLOTS, first, 0)

    total = got_ref[0]
    for i in range(1, got_ref.shape[0]):
        total = total + got_ref[i]
    cosine, sine = total[:n_lines], total[n_lines:]
    triples = half_space(trip_ref[...])
    table = [
        (2.0 * math.pi) * jnp.concatenate(lines(triples[d : d + 1]), axis=0).astype(jnp.float32)
        for d in range(3)
    ]
    norm = table[0] * table[0] + table[1] * table[1] + table[2] * table[2]
    damping = 4.0 * math.pi * jnp.exp(-norm / 1600000.0) / norm
    energy = scale * jnp.sum(damping * (cosine * cosine + sine * sine))
    for kind, rows in enumerate([damping * cosine, damping * sine] + table):
        stage[kind * n_lines : (kind + 1) * n_lines] = rows
    for move in to_scalars(stage, w, w_sem):
        move.start()
    for move in to_scalars(stage, w, w_sem):
        move.wait()
    zero = jnp.zeros((ROWS, 128), jnp.float32)

    def block(b, carry):
        def part(p, state):
            t = b * parts + p
            slot = lax.rem(t, SLOTS)
            copy(slot, b, p).wait()

            def mode(i, state):
                f0, f1, f2, pot = state
                k = p * PART + i
                wr, wi = w[k], w[modes + k]
                c = ring[slot, i, 0]
                s = ring[slot, i, 1]
                pot = pot + (wr * c + wi * s)
                g = wr * s - wi * c
                return (
                    f0 + w[2 * modes + k] * g,
                    f1 + w[3 * modes + k] * g,
                    f2 + w[4 * modes + k] * g,
                    pot,
                )

            state = lax.fori_loop(0, PART, mode, state, unroll=UNROLL)

            @pl.when(t + SLOTS < blocks * parts)
            def _():
                fetch(t + SLOTS)

            return state

        state = lax.fori_loop(0, parts, part, (zero,) * 4)
        for t in range(2):
            for c in range(4):
                o_ref[2 * b + t, HALF * c : HALF * (c + 1)] = state[c][HALF * t : HALF * (t + 1)]
            o_ref[2 * b + t, 4 * HALF :] = jnp.full((8, 128), energy, jnp.float32)
        return carry

    lax.fori_loop(0, blocks, block, 0)


def on_device(scaled_coordinate_array, particle_charge_list, reciprocal_triples):
    local_atoms = scaled_coordinate_array.shape[1]
    modes = reciprocal_triples.shape[1]
    n_atom = lax.axis_size("atom")
    n_kvec = lax.axis_size("kvec")
    natoms = local_atoms * n_atom
    blocks = local_atoms // BLOCK
    n_lines = modes // 128
    q = particle_charge_list.reshape(local_atoms // 128, 128)

    vmem = pl.BlockSpec(memory_space=pltpu.VMEM)
    hbm = pl.BlockSpec(memory_space=pl.ANY)
    def ring(slots, part):
        return [
            pltpu.VMEM((slots, part, 2, ROWS, 128), jnp.float32),
            pltpu.SemaphoreType.DMA((slots,)),
        ]

    def scalars(dtype):
        return [
            pltpu.VMEM((KINDS * n_lines, 128), dtype),
            pltpu.SMEM((KINDS * modes,), dtype),
            pltpu.SemaphoreType.DMA((KINDS * n_lines,)),
        ]

    positive = pltpu.VMEM(((TOP + 1) * ROWS, 128), jnp.float32)
    both = pltpu.VMEM(((2 * TOP + 1) * ROWS, 128), jnp.float32)
    e, share = pl.pallas_call(
        phases_kernel,
        in_specs=[hbm, hbm, hbm],
        out_specs=[hbm, vmem],
        out_shape=[
            jax.ShapeDtypeStruct((blocks, modes, 2, ROWS, 128), jnp.float32),
            jax.ShapeDtypeStruct((8, 128), jnp.float32),
        ],
        scratch_shapes=[
            positive,
            positive,
            positive,
            both,
            positive,
            both,
            pltpu.VMEM((modes * 8, 128), jnp.float32),
            pltpu.VMEM((modes * 8, 128), jnp.float32),
            pltpu.VMEM((3, modes), jnp.int32),
            pltpu.VMEM((3, local_atoms), jnp.float32),
            pltpu.VMEM((local_atoms // 128, 128), jnp.float32),
            pltpu.SemaphoreType.DMA((3,)),
            pltpu.VMEM((3, local_atoms // 128, 128), jnp.float32),
        ]
        + scalars(jnp.int32)
        + ring(WRITE_SLOTS, WRITE_PART),
        compiler_params=pltpu.CompilerParams(vmem_limit_bytes=48 * MIB),
    )(reciprocal_triples, scaled_coordinate_array, q)

    share = share + lax.ppermute(share, "atom", [(i, i ^ 1) for i in range(n_atom)])
    share = jnp.broadcast_to(share[None], (n_atom // 2, 8, 128))
    cores = [[c + 2 * m for m in range(n_atom // 2)] for c in range(2)]
    got = lax.all_to_all(share, "atom", 0, 0, tiled=True, axis_index_groups=cores)

    terms = pl.pallas_call(
        functools.partial(response_kernel, 50.0 / natoms),
        in_specs=[vmem, vmem, hbm],
        out_specs=vmem,
        out_shape=jax.ShapeDtypeStruct((n_kvec, 4 * HALF + 8, 128), jnp.float32),
        scratch_shapes=scalars(jnp.float32) + ring(SLOTS, PART),
        compiler_params=pltpu.CompilerParams(vmem_limit_bytes=24 * MIB),
    )(got, reciprocal_triples, e)

    own = lax.all_to_all(terms, "kvec", 0, 0, tiled=True).sum(axis=0)
    energy = own[4 * HALF, 0]
    copies = jnp.broadcast_to(own[None, : 4 * HALF], (n_kvec, 4 * HALF, 128))
    summed = lax.all_to_all(copies, "kvec", 0, 0, tiled=True)
    summed = summed.reshape(n_kvec, 4, HALF * 128).transpose(1, 0, 2).reshape(4, local_atoms)
    scale = 1.0 / math.sqrt(natoms)
    forces = summed[:3] * scale
    potential = summed[3] * (400.0 * scale) / nonzero(particle_charge_list)
    return (forces, potential, energy)


def solution(mesh):
    return jax.shard_map(
        on_device,
        mesh=mesh,
        in_specs=(P(None, "atom"), P("atom"), P(None, "kvec")),
        out_specs=(P(None, "atom"), P("atom"), P()),
        check_vma=False,
    )
```

```python
import functools
import math

import jax
import jax.numpy as jnp
from jax import lax
from jax.experimental import pallas as pl
from jax.experimental.pallas import tpu as pltpu
from jax.sharding import PartitionSpec as P

TOP = 128
STRIDE = 16
BLOCK = 4096
ROWS = BLOCK // 128
HALF = ROWS // 2
PART = 32
SLOTS = 12
WRITE_PART = 64
WRITE_SLOTS = 5
UNROLL = 16
GROUP = 8
TINY = 1e-6
KINDS = 5
MIB = 1 << 20


def rows_of(ref, start):
    return ref[pl.ds(pl.multiple_of(start, ROWS), ROWS), :]


def times(a, b):
    return a[0] * b[0] - a[1] * b[1], a[0] * b[1] + a[1] * b[0]


def turn(x):
    y = 4.0 * (x - jnp.round(x))
    n = jnp.round(y)
    r = (0.5 * math.pi) * (y - n)
    z = r * r
    s = r + r * z * (-1.6666654611e-1 + z * (8.3321608736e-3 - 1.9515295891e-4 * z))
    c = 4.166664568298827e-2 + z * (-1.388731625493765e-3 + 2.443315711809948e-5 * z)
    c = 1.0 + z * (c * z - 0.5)
    odd = jnp.abs(n) == 1.0
    cos = jnp.where(odd, s, c)
    sin = jnp.where(odd, c, s)
    cos = jnp.where((n > 0.5) | (n < -1.5), -cos, cos)
    sin = jnp.where((n > 1.5) | (n < -0.5), -sin, sin)
    return cos, sin


def fill_powers(x, weight, low, cos_ref, sin_ref, signed):
    small = [(jnp.ones_like(x), jnp.zeros_like(x)), turn(x)]
    for b in range(2, STRIDE // 2 + 1):
        small.append(times(small[b // 2], small[b - b // 2]))
    big = times(small[-1], small[-1])

    def put(h, c, s):
        def at(r):
            return pl.ds(pl.multiple_of(r * ROWS + low, 8), HALF)

        cos_ref[at(h)] = c
        if signed:
            sin_ref[at(TOP + h)] = s
            sin_ref[at(TOP - h)] = -s
        else:
            sin_ref[at(h)] = s

    def weighted(v):
        return v if weight is None else (weight * v[0], weight * v[1])

    for b in range(STRIDE // 2):
        put(b, *weighted(small[b]))

    def around(a, state, both):
        c, s = state
        put(STRIDE * a, c, s)
        for b in range(1, STRIDE // 2 + 1):
            cb, sb = small[b]
            cc, ss, sc, cs = c * cb, s * sb, s * cb, c * sb
            put(STRIDE * a - b, cc + ss, sc - cs)
            if both and b < STRIDE // 2:
                put(STRIDE * a + b, cc - ss, sc + cs)

    def step(a, state):
        around(a, state, True)
        return times(state, big)

    last = lax.fori_loop(1, TOP // STRIDE, step, weighted(big), unroll=TOP // STRIDE - 1)
    around(TOP // STRIDE, last, False)


def eighths(v):
    return (v[0:8] + v[8:16]) + (v[16:24] + v[24:32])


def nonzero(q):
    return jnp.where(jnp.abs(q) < TINY, TINY, q)


def lines(v):
    return [v[:, at : at + 128] for at in range(0, v.shape[1], 128)]


def to_scalars(stage, scalars, sems):
    return [
        pltpu.make_async_copy(stage.at[i], scalars.at[pl.ds(128 * i, 128)], sems.at[i])
        for i in range(stage.shape[0])
    ]


def half_space(triples):
    return jnp.where(triples[0:1] < 0, -triples, triples)


def phases_kernel(
    trip_hbm, x_hbm, q_hbm, e_ref, s_ref,
    xc, xs, yc, ys, zc, zs, acc_c, acc_s, trip_ref, x_ref, q_ref, in_sems,
    xyz, stage, idx, idx_sem, ring, sems,
):
    blocks, modes = e_ref.shape[0], e_ref.shape[1]
    parts = modes // WRITE_PART
    loads = [
        pltpu.make_async_copy(src, dst, in_sems.at[i])
        for i, (src, dst) in enumerate(((x_hbm, x_ref), (q_hbm, q_ref), (trip_hbm, trip_ref)))
    ]
    for load in loads:
        load.start()

    def clear(i, carry):
        at = pl.ds(pl.multiple_of(i * 128, 128), 128)
        acc_c[at] = jnp.zeros((128, 128), jnp.float32)
        acc_s[at] = jnp.zeros((128, 128), jnp.float32)
        return carry

    lax.fori_loop(0, acc_c.shape[0] // 128, clear, 0)
    for load in loads:
        load.wait()
    triples = half_space(trip_ref[...])
    h, k, l = triples[0:1], triples[1:2], triples[2:3]
    for kind, row in enumerate((h, jnp.abs(k), k + TOP, jnp.abs(l), l + TOP)):
        for r, line in enumerate(lines(ROWS * row)):
            at = kind * (modes // 128) + r
            stage[at : at + 1] = line
    for move in to_scalars(stage, idx, idx_sem):
        move.start()

    def fold(i, carry):
        for d in range(3):
            xyz[d, pl.ds(i, 1)] = x_ref[d : d + 1, pl.ds(pl.multiple_of(i * 128, 128), 128)]
        return carry

    lax.fori_loop(0, xyz.shape[1], fold, 0, unroll=16)
    faint = jnp.max(jnp.where(jnp.abs(q_ref[...]) < TINY, 1.0, 0.0)) > 0.0

    def copy(slot, b, p):
        return pltpu.make_async_copy(
            ring.at[slot], e_ref.at[b, pl.ds(p * WRITE_PART, WRITE_PART)], sems.at[slot]
        )

    def block(b, carry):
        for low in (0, HALF):
            here = pl.ds(pl.multiple_of(b * ROWS + low, HALF), HALF)
            for d, (c_ref, s_ref_) in enumerate(((xc, xs), (yc, ys), (zc, zs))):
                weight = nonzero(q_ref[here]) if d == 2 else None
                fill_powers(xyz[d, here], weight, low, c_ref, s_ref_, d > 0)

        @pl.when(b == 0)
        def _():
            for move in to_scalars(stage, idx, idx_sem):
                move.wait()

        def part(p, carry):
            t = b * parts + p
            slot = lax.rem(t, WRITE_SLOTS)

            @pl.when(t >= WRITE_SLOTS)
            def _():
                copy(slot, b, p).wait()

            def group(g, ratio):
                sums_c, sums_s = [], []
                for j in range(GROUP):
                    i = g * GROUP + j
                    k = p * WRITE_PART + i
                    h = idx[k]
                    first = rows_of(xc, h), rows_of(xs, h)
                    second = rows_of(yc, idx[modes + k]), rows_of(ys, idx[2 * modes + k])
                    third = rows_of(zc, idx[3 * modes + k]), rows_of(zs, idx[4 * modes + k])
                    c, s = times(times(first, second), third)
                    ring[slot, i, 0] = c
                    ring[slot, i, 1] = s
                    if ratio is not None:
                        c, s = ratio * c, ratio * s
                    sums_c.append(eighths(c))
                    sums_s.append(eighths(s))
                at = pl.ds(pl.multiple_of((p * WRITE_PART + g * GROUP) * 8, 8 * GROUP), 8 * GROUP)
                sums_c = acc_c[at] + jnp.concatenate(sums_c, axis=0)
                sums_s = acc_s[at] + jnp.concatenate(sums_s, axis=0)
                acc_c[at] = sums_c
                acc_s[at] = sums_s

            groups = WRITE_PART // GROUP

            @pl.when(faint)
            def _():
                q = q_ref[pl.ds(pl.multiple_of(b * ROWS, ROWS), ROWS)]
                ratio = q / nonzero(q)
                lax.fori_loop(0, groups, lambda g, c: (group(g, ratio), c)[1], 0)

            @pl.when(jnp.logical_not(faint))
            def _():
                lax.fori_loop(0, groups, lambda g, c: (group(g, None), c)[1], 0, unroll=UNROLL // GROUP)

            copy(slot, b, p).start()
            return carry

        return lax.fori_loop(0, parts, part, carry)

    lax.fori_loop(0, blocks, block, 0)

    for half, acc in enumerate((acc_c, acc_s)):
        for r in range(modes // 128):
            rows = acc[pl.ds(1024 * r, 128, stride=8)]
            for sub in range(1, 8):
                rows = rows + acc[pl.ds(1024 * r + sub, 128, stride=8)]
            at = half * (modes // 128) + r
            s_ref[at : at + 1] = jnp.sum(rows.T, axis=0, keepdims=True)

    def drain(slot, carry):
        copy(slot, 0, 0).wait()
        return carry

    lax.fori_loop(0, WRITE_SLOTS, drain, 0)


def response_kernel(scale, got_ref, trip_ref, e_ref, o_ref, stage, w, w_sem, ring, sems):
    blocks, modes = e_ref.shape[0], e_ref.shape[1]
    parts = modes // PART
    n_lines = modes // 128

    def copy(slot, b, p):
        return pltpu.make_async_copy(
            e_ref.at[b, pl.ds(p * PART, PART)], ring.at[slot], sems.at[slot]
        )

    def fetch(t):
        copy(lax.rem(t, SLOTS), t // parts, lax.rem(t, parts)).start()

    def first(t, carry):
        fetch(t)
        return carry

    lax.fori_loop(0, SLOTS, first, 0)

    total = got_ref[0]
    for i in range(1, got_ref.shape[0]):
        total = total + got_ref[i]
    cosine, sine = total[:n_lines], total[n_lines:]
    triples = half_space(trip_ref[...])
    table = [
        (2.0 * math.pi) * jnp.concatenate(lines(triples[d : d + 1]), axis=0).astype(jnp.float32)
        for d in range(3)
    ]
    norm = table[0] * table[0] + table[1] * table[1] + table[2] * table[2]
    damping = 4.0 * math.pi * jnp.exp(-norm / 1600000.0) / norm
    energy = scale * jnp.sum(damping * (cosine * cosine + sine * sine))
    for kind, rows in enumerate([damping * cosine, damping * sine] + table):
        stage[kind * n_lines : (kind + 1) * n_lines] = rows
    for move in to_scalars(stage, w, w_sem):
        move.start()
    for move in to_scalars(stage, w, w_sem):
        move.wait()
    zero = jnp.zeros((ROWS, 128), jnp.float32)

    def block(b, carry):
        def part(p, state):
            t = b * parts + p
            slot = lax.rem(t, SLOTS)
            copy(slot, b, p).wait()

            def mode(i, state):
                f0, f1, f2, pot = state
                k = p * PART + i
                wr, wi = w[k], w[modes + k]
                c = ring[slot, i, 0]
                s = ring[slot, i, 1]
                pot = pot + (wr * c + wi * s)
                g = wr * s - wi * c
                return (
                    f0 + w[2 * modes + k] * g,
                    f1 + w[3 * modes + k] * g,
                    f2 + w[4 * modes + k] * g,
                    pot,
                )

            state = lax.fori_loop(0, PART, mode, state, unroll=UNROLL)

            @pl.when(t + SLOTS < blocks * parts)
            def _():
                fetch(t + SLOTS)

            return state

        state = lax.fori_loop(0, parts, part, (zero,) * 4)
        for t in range(2):
            for c in range(4):
                o_ref[2 * b + t, HALF * c : HALF * (c + 1)] = state[c][HALF * t : HALF * (t + 1)]
            o_ref[2 * b + t, 4 * HALF :] = jnp.full((8, 128), energy, jnp.float32)
        return carry

    lax.fori_loop(0, blocks, block, 0)


def on_device(scaled_coordinate_array, particle_charge_list, reciprocal_triples):
    local_atoms = scaled_coordinate_array.shape[1]
    modes = reciprocal_triples.shape[1]
    n_atom = lax.axis_size("atom")
    n_kvec = lax.axis_size("kvec")
    natoms = local_atoms * n_atom
    blocks = local_atoms // BLOCK
    n_lines = modes // 128
    q = particle_charge_list.reshape(local_atoms // 128, 128)

    vmem = pl.BlockSpec(memory_space=pltpu.VMEM)
    hbm = pl.BlockSpec(memory_space=pltpu.HBM)
    def ring(slots, part):
        return [
            pltpu.VMEM((slots, part, 2, ROWS, 128), jnp.float32),
            pltpu.SemaphoreType.DMA((slots,)),
        ]

    def scalars(dtype):
        return [
            pltpu.VMEM((KINDS * n_lines, 128), dtype),
            pltpu.SMEM((KINDS * modes,), dtype),
            pltpu.SemaphoreType.DMA((KINDS * n_lines,)),
        ]

    positive = pltpu.VMEM(((TOP + 1) * ROWS, 128), jnp.float32)
    both = pltpu.VMEM(((2 * TOP + 1) * ROWS, 128), jnp.float32)
    e, share = pl.pallas_call(
        phases_kernel,
        in_specs=[hbm, hbm, hbm],
        out_specs=[hbm, vmem],
        out_shape=[
            jax.ShapeDtypeStruct((blocks, modes, 2, ROWS, 128), jnp.float32),
            pltpu.VMEM((8, 128), jnp.float32),
        ],
        scratch_shapes=[
            positive,
            positive,
            positive,
            both,
            positive,
            both,
            pltpu.VMEM((modes * 8, 128), jnp.float32),
            pltpu.VMEM((modes * 8, 128), jnp.float32),
            pltpu.VMEM((3, modes), jnp.int32),
            pltpu.VMEM((3, local_atoms), jnp.float32),
            pltpu.VMEM((local_atoms // 128, 128), jnp.float32),
            pltpu.SemaphoreType.DMA((3,)),
            pltpu.VMEM((3, local_atoms // 128, 128), jnp.float32),
        ]
        + scalars(jnp.int32)
        + ring(WRITE_SLOTS, WRITE_PART),
        compiler_params=pltpu.CompilerParams(vmem_limit_bytes=58 * MIB),
    )(reciprocal_triples, scaled_coordinate_array, q)

    share = share + lax.ppermute(share, "atom", [(i, i ^ 1) for i in range(n_atom)])
    share = jnp.broadcast_to(share[None], (n_atom // 2, 8, 128))
    cores = [[c + 2 * m for m in range(n_atom // 2)] for c in range(2)]
    got = lax.all_to_all(share, "atom", 0, 0, tiled=True, axis_index_groups=cores)

    terms = pl.pallas_call(
        functools.partial(response_kernel, 50.0 / natoms),
        in_specs=[vmem, vmem, hbm],
        out_specs=vmem,
        out_shape=jax.ShapeDtypeStruct((n_kvec, 4 * HALF + 8, 128), jnp.float32),
        scratch_shapes=scalars(jnp.float32) + ring(SLOTS, PART),
        compiler_params=pltpu.CompilerParams(vmem_limit_bytes=32 * MIB),
    )(got, reciprocal_triples, e)

    own = lax.all_to_all(terms, "kvec", 0, 0, tiled=True).sum(axis=0)
    energy = own[4 * HALF, 0]
    copies = jnp.broadcast_to(own[None, : 4 * HALF], (n_kvec, 4 * HALF, 128))
    summed = lax.all_to_all(copies, "kvec", 0, 0, tiled=True)
    summed = summed.reshape(n_kvec, 4, HALF * 128).transpose(1, 0, 2).reshape(4, local_atoms)
    scale = 1.0 / math.sqrt(natoms)
    forces = summed[:3] * scale
    potential = summed[3] * (400.0 * scale) / nonzero(particle_charge_list)
    return (forces, potential, energy)


def solution(mesh):
    return jax.shard_map(
        on_device,
        mesh=mesh,
        in_specs=(P(None, "atom"), P("atom"), P(None, "kvec")),
        out_specs=(P(None, "atom"), P("atom"), P()),
        check_vma=False,
    )
```

```python
import functools
import math

import jax
import jax.numpy as jnp
from jax import lax
from jax.experimental import pallas as pl
from jax.experimental.pallas import tpu as pltpu
from jax.sharding import PartitionSpec as P

TOP = 128
STRIDE = 16
BLOCK = 4096
ROWS = BLOCK // 128
HALF = ROWS // 2
PART = 32
SLOTS = 12
WRITE_PART = 64
WRITE_SLOTS = 5
KEEP = 64
UNROLL = 16
GROUP = 8
TINY = 1e-6
KINDS = 5
MIB = 1 << 20


def rows_of(ref, start):
    return ref[pl.ds(pl.multiple_of(start, ROWS), ROWS), :]


def times(a, b):
    return a[0] * b[0] - a[1] * b[1], a[0] * b[1] + a[1] * b[0]


def turn(x):
    y = 4.0 * (x - jnp.round(x))
    n = jnp.round(y)
    r = (0.5 * math.pi) * (y - n)
    z = r * r
    s = r + r * z * (-1.6666654611e-1 + z * (8.3321608736e-3 - 1.9515295891e-4 * z))
    c = 4.166664568298827e-2 + z * (-1.388731625493765e-3 + 2.443315711809948e-5 * z)
    c = 1.0 + z * (c * z - 0.5)
    odd = jnp.abs(n) == 1.0
    cos = jnp.where(odd, s, c)
    sin = jnp.where(odd, c, s)
    cos = jnp.where((n > 0.5) | (n < -1.5), -cos, cos)
    sin = jnp.where((n > 1.5) | (n < -0.5), -sin, sin)
    return cos, sin


def fill_powers(x, weight, low, cos_ref, sin_ref, signed):
    small = [(jnp.ones_like(x), jnp.zeros_like(x)), turn(x)]
    for b in range(2, STRIDE // 2 + 1):
        small.append(times(small[b // 2], small[b - b // 2]))
    big = times(small[-1], small[-1])

    def put(h, c, s):
        def at(r):
            return pl.ds(pl.multiple_of(r * ROWS + low, 8), HALF)

        cos_ref[at(h)] = c
        if signed:
            sin_ref[at(TOP + h)] = s
            sin_ref[at(TOP - h)] = -s
        else:
            sin_ref[at(h)] = s

    def weighted(v):
        return v if weight is None else (weight * v[0], weight * v[1])

    for b in range(STRIDE // 2):
        put(b, *weighted(small[b]))

    def around(a, state, both):
        c, s = state
        put(STRIDE * a, c, s)
        for b in range(1, STRIDE // 2 + 1):
            cb, sb = small[b]
            cc, ss, sc, cs = c * cb, s * sb, s * cb, c * sb
            put(STRIDE * a - b, cc + ss, sc - cs)
            if both and b < STRIDE // 2:
                put(STRIDE * a + b, cc - ss, sc + cs)

    def step(a, state):
        around(a, state, True)
        return times(state, big)

    last = lax.fori_loop(1, TOP // STRIDE, step, weighted(big), unroll=TOP // STRIDE - 1)
    around(TOP // STRIDE, last, False)


def eighths(v):
    return (v[0:8] + v[8:16]) + (v[16:24] + v[24:32])


def nonzero(q):
    return jnp.where(jnp.abs(q) < TINY, TINY, q)


def lines(v):
    return [v[:, at : at + 128] for at in range(0, v.shape[1], 128)]


def to_scalars(stage, scalars, sems):
    return [
        pltpu.make_async_copy(stage.at[i], scalars.at[pl.ds(128 * i, 128)], sems.at[i])
        for i in range(stage.shape[0])
    ]


def half_space(triples):
    return jnp.where(triples[0:1] < 0, -triples, triples)


def phases_kernel(
    trip_hbm, x_hbm, q_hbm, e_ref, s_ref, keep_ref, modes_ref,
    xc, xs, yc, ys, zc, zs, acc_c, acc_s, trip_ref, x_ref, q_ref, in_sems,
    xyz, stage, idx, idx_sem, ring, sems,
):
    blocks, modes = e_ref.shape[0], e_ref.shape[1]
    parts = modes // WRITE_PART
    loads = [
        pltpu.make_async_copy(src, dst, in_sems.at[i])
        for i, (src, dst) in enumerate(((x_hbm, x_ref), (q_hbm, q_ref), (trip_hbm, trip_ref)))
    ]
    for load in loads:
        load.start()

    def clear(i, carry):
        at = pl.ds(pl.multiple_of(i * 128, 128), 128)
        acc_c[at] = jnp.zeros((128, 128), jnp.float32)
        acc_s[at] = jnp.zeros((128, 128), jnp.float32)
        return carry

    lax.fori_loop(0, acc_c.shape[0] // 128, clear, 0)
    for load in loads:
        load.wait()
    triples = half_space(trip_ref[...])
    h, k, l = triples[0:1], triples[1:2], triples[2:3]
    for kind, row in enumerate((h, jnp.abs(k), k + TOP, jnp.abs(l), l + TOP)):
        for r, line in enumerate(lines(ROWS * row)):
            at = kind * (modes // 128) + r
            stage[at : at + 1] = line
    for move in to_scalars(stage, idx, idx_sem):
        move.start()
    n_lines = modes // 128
    table = [
        (2.0 * math.pi) * jnp.concatenate(lines(triples[d : d + 1]), axis=0).astype(jnp.float32)
        for d in range(3)
    ]
    norm = table[0] * table[0] + table[1] * table[1] + table[2] * table[2]
    modes_ref[:n_lines] = 4.0 * math.pi * jnp.exp(-norm / 1600000.0) / norm
    for d in range(3):
        modes_ref[n_lines * (d + 1) : n_lines * (d + 2)] = table[d]

    def fold(i, carry):
        for d in range(3):
            xyz[d, pl.ds(i, 1)] = x_ref[d : d + 1, pl.ds(pl.multiple_of(i * 128, 128), 128)]
        return carry

    lax.fori_loop(0, xyz.shape[1], fold, 0, unroll=16)
    faint = jnp.max(jnp.where(jnp.abs(q_ref[...]) < TINY, 1.0, 0.0)) > 0.0

    def copy(slot, b, p):
        return pltpu.make_async_copy(
            ring.at[slot], e_ref.at[b, pl.ds(p * WRITE_PART, WRITE_PART)], sems.at[slot]
        )

    def block(b, carry):
        for low in (0, HALF):
            here = pl.ds(pl.multiple_of(b * ROWS + low, HALF), HALF)
            for d, (c_ref, s_ref_) in enumerate(((xc, xs), (yc, ys), (zc, zs))):
                weight = nonzero(q_ref[here]) if d == 2 else None
                fill_powers(xyz[d, here], weight, low, c_ref, s_ref_, d > 0)

        @pl.when(b == 0)
        def _():
            for move in to_scalars(stage, idx, idx_sem):
                move.wait()

        def part(p, carry):
            t = b * parts + p
            slot = lax.rem(t, WRITE_SLOTS)

            @pl.when(t >= WRITE_SLOTS)
            def _():
                copy(slot, b, p).wait()

            run(ring.at[slot], b, p * WRITE_PART)
            copy(slot, b, p).start()
            return carry

        kept = jnp.where(b == blocks - 1, KEEP // WRITE_PART, 0)
        return lax.fori_loop(0, parts - kept, part, carry)

    def run(out, b, start):
        def group(g, ratio):
            sums_c, sums_s = [], []
            for j in range(GROUP):
                i = g * GROUP + j
                k = start + i
                h = idx[k]
                first = rows_of(xc, h), rows_of(xs, h)
                second = rows_of(yc, idx[modes + k]), rows_of(ys, idx[2 * modes + k])
                third = rows_of(zc, idx[3 * modes + k]), rows_of(zs, idx[4 * modes + k])
                c, s = times(times(first, second), third)
                out[i, 0] = c
                out[i, 1] = s
                if ratio is not None:
                    c, s = ratio * c, ratio * s
                sums_c.append(eighths(c))
                sums_s.append(eighths(s))
            at = pl.ds(pl.multiple_of((start + g * GROUP) * 8, 8 * GROUP), 8 * GROUP)
            sums_c = acc_c[at] + jnp.concatenate(sums_c, axis=0)
            sums_s = acc_s[at] + jnp.concatenate(sums_s, axis=0)
            acc_c[at] = sums_c
            acc_s[at] = sums_s

        groups = out.shape[0] // GROUP

        @pl.when(faint)
        def _():
            q = q_ref[pl.ds(pl.multiple_of(b * ROWS, ROWS), ROWS)]
            ratio = q / nonzero(q)
            lax.fori_loop(0, groups, lambda g, c: (group(g, ratio), c)[1], 0)

        @pl.when(jnp.logical_not(faint))
        def _():
            lax.fori_loop(
                0, groups, lambda g, c: (group(g, None), c)[1], 0, unroll=UNROLL // GROUP
            )

    lax.fori_loop(0, blocks, block, 0)
    run(keep_ref, blocks - 1, modes - KEEP)

    for half, acc in enumerate((acc_c, acc_s)):
        for r in range(modes // 128):
            rows = acc[pl.ds(1024 * r, 128, stride=8)]
            for sub in range(1, 8):
                rows = rows + acc[pl.ds(1024 * r + sub, 128, stride=8)]
            at = half * (modes // 128) + r
            s_ref[at : at + 1] = jnp.sum(rows.T, axis=0, keepdims=True)

    def drain(slot, carry):
        copy(slot, 0, 0).wait()
        return carry

    lax.fori_loop(0, WRITE_SLOTS, drain, 0)


def response_kernel(scale, got_ref, modes_ref, keep_ref, e_ref, o_ref, stage, w, w_sem, ring, sems):
    blocks, modes = e_ref.shape[0], e_ref.shape[1]
    parts = modes // PART
    n_lines = modes // 128
    lead = (modes - KEEP) // PART
    n_parts = blocks * parts - KEEP // PART

    def copy(slot, b, p):
        return pltpu.make_async_copy(
            e_ref.at[b, pl.ds(p * PART, PART)], ring.at[slot], sems.at[slot]
        )

    def fetch(t):
        later = t - lead
        b = jnp.where(later < 0, blocks - 1, later // parts)
        copy(lax.rem(t, SLOTS), b, jnp.where(later < 0, t, lax.rem(later, parts))).start()

    def first(t, carry):
        fetch(t)
        return carry

    lax.fori_loop(0, SLOTS, first, 0)

    total = got_ref[0]
    for i in range(1, got_ref.shape[0]):
        total = total + got_ref[i]
    cosine, sine = total[:n_lines], total[n_lines:]
    damping = modes_ref[:n_lines]
    energy = scale * jnp.sum(damping * (cosine * cosine + sine * sine))
    stage[:n_lines] = damping * cosine
    stage[n_lines : 2 * n_lines] = damping * sine
    stage[2 * n_lines :] = modes_ref[n_lines:]
    for move in to_scalars(stage, w, w_sem):
        move.start()
    for move in to_scalars(stage, w, w_sem):
        move.wait()
    zero = jnp.zeros((ROWS, 128), jnp.float32)

    def run(source, start, state):
        def mode(i, state):
            f0, f1, f2, pot = state
            k = start + i
            wr, wi = w[k], w[modes + k]
            c = source[i, 0]
            s = source[i, 1]
            pot = pot + (wr * c + wi * s)
            g = wr * s - wi * c
            return (
                f0 + w[2 * modes + k] * g,
                f1 + w[3 * modes + k] * g,
                f2 + w[4 * modes + k] * g,
                pot,
            )

        return lax.fori_loop(0, source.shape[0], mode, state, unroll=UNROLL)

    def stream(b, before, count, state):
        def part(p, state):
            t = before + p
            slot = lax.rem(t, SLOTS)
            copy(slot, b, p).wait()
            state = run(ring.at[slot], p * PART, state)

            @pl.when(t + SLOTS < n_parts)
            def _():
                fetch(t + SLOTS)

            return state

        state = lax.fori_loop(0, count, part, state)
        for t in range(2):
            for c in range(4):
                o_ref[2 * b + t, HALF * c : HALF * (c + 1)] = state[c][HALF * t : HALF * (t + 1)]
            o_ref[2 * b + t, 4 * HALF :] = jnp.full((8, 128), energy, jnp.float32)

    stream(blocks - 1, 0, lead, run(keep_ref, modes - KEEP, (zero,) * 4))

    def block(b, carry):
        stream(b, lead + b * parts, parts, (zero,) * 4)
        return carry

    lax.fori_loop(0, blocks - 1, block, 0)


def on_device(scaled_coordinate_array, particle_charge_list, reciprocal_triples):
    local_atoms = scaled_coordinate_array.shape[1]
    modes = reciprocal_triples.shape[1]
    n_atom = lax.axis_size("atom")
    n_kvec = lax.axis_size("kvec")
    natoms = local_atoms * n_atom
    blocks = local_atoms // BLOCK
    n_lines = modes // 128
    q = particle_charge_list.reshape(local_atoms // 128, 128)

    vmem = pl.BlockSpec(memory_space=pltpu.VMEM)
    hbm = pl.BlockSpec(memory_space=pltpu.HBM)
    def ring(slots, part):
        return [
            pltpu.VMEM((slots, part, 2, ROWS, 128), jnp.float32),
            pltpu.SemaphoreType.DMA((slots,)),
        ]

    def scalars(dtype):
        return [
            pltpu.VMEM((KINDS * n_lines, 128), dtype),
            pltpu.SMEM((KINDS * modes,), dtype),
            pltpu.SemaphoreType.DMA((KINDS * n_lines,)),
        ]

    positive = pltpu.VMEM(((TOP + 1) * ROWS, 128), jnp.float32)
    both = pltpu.VMEM(((2 * TOP + 1) * ROWS, 128), jnp.float32)
    e, share, keep, spectrum = pl.pallas_call(
        phases_kernel,
        in_specs=[hbm, hbm, hbm],
        out_specs=[hbm, vmem, vmem, vmem],
        out_shape=[
            jax.ShapeDtypeStruct((blocks, modes, 2, ROWS, 128), jnp.float32),
            pltpu.VMEM((8, 128), jnp.float32),
            pltpu.VMEM((KEEP, 2, ROWS, 128), jnp.float32),
            pltpu.VMEM((4 * n_lines, 128), jnp.float32),
        ],
        scratch_shapes=[
            positive,
            positive,
            positive,
            both,
            positive,
            both,
            pltpu.VMEM((modes * 8, 128), jnp.float32),
            pltpu.VMEM((modes * 8, 128), jnp.float32),
            pltpu.VMEM((3, modes), jnp.int32),
            pltpu.VMEM((3, local_atoms), jnp.float32),
            pltpu.VMEM((local_atoms // 128, 128), jnp.float32),
            pltpu.SemaphoreType.DMA((3,)),
            pltpu.VMEM((3, local_atoms // 128, 128), jnp.float32),
        ]
        + scalars(jnp.int32)
        + ring(WRITE_SLOTS, WRITE_PART),
        compiler_params=pltpu.CompilerParams(vmem_limit_bytes=58 * MIB),
    )(reciprocal_triples, scaled_coordinate_array, q)

    share = share + lax.ppermute(share, "atom", [(i, i ^ 1) for i in range(n_atom)])
    share = jnp.broadcast_to(share[None], (n_atom // 2, 8, 128))
    cores = [[c + 2 * m for m in range(n_atom // 2)] for c in range(2)]
    got = lax.all_to_all(share, "atom", 0, 0, tiled=True, axis_index_groups=cores)

    terms = pl.pallas_call(
        functools.partial(response_kernel, 50.0 / natoms),
        in_specs=[vmem, vmem, vmem, hbm],
        out_specs=vmem,
        out_shape=jax.ShapeDtypeStruct((n_kvec, 4 * HALF + 8, 128), jnp.float32),
        scratch_shapes=scalars(jnp.float32) + ring(SLOTS, PART),
        compiler_params=pltpu.CompilerParams(vmem_limit_bytes=32 * MIB),
    )(got, spectrum, keep, e)

    own = lax.all_to_all(terms, "kvec", 0, 0, tiled=True).sum(axis=0)
    energy = own[4 * HALF, 0]
    copies = jnp.broadcast_to(own[None, : 4 * HALF], (n_kvec, 4 * HALF, 128))
    summed = lax.all_to_all(copies, "kvec", 0, 0, tiled=True)
    summed = summed.reshape(n_kvec, 4, HALF * 128).transpose(1, 0, 2).reshape(4, local_atoms)
    scale = 1.0 / math.sqrt(natoms)
    forces = summed[:3] * scale
    potential = summed[3] * (400.0 * scale) / nonzero(particle_charge_list)
    return (forces, potential, energy)


def solution(mesh):
    return jax.shard_map(
        on_device,
        mesh=mesh,
        in_specs=(P(None, "atom"), P("atom"), P(None, "kvec")),
        out_specs=(P(None, "atom"), P("atom"), P()),
        check_vma=False,
    )
```

```python
import functools
import math

import jax
import jax.numpy as jnp
from jax import lax
from jax.experimental import pallas as pl
from jax.experimental.pallas import tpu as pltpu
from jax.sharding import PartitionSpec as P

TOP = 128
STRIDE = 16
BLOCK = 4096
ROWS = BLOCK // 128
HALF = ROWS // 2
PART = 32
SLOTS = 12
WRITE_PART = 64
WRITE_SLOTS = 5
KEEP = 64
UNROLL = 16
GROUP = 8
TINY = 1e-6
KINDS = 5
MIB = 1 << 20


def rows_of(ref, start):
    return ref[pl.ds(pl.multiple_of(start, ROWS), ROWS), :]


def times(a, b):
    return a[0] * b[0] - a[1] * b[1], a[0] * b[1] + a[1] * b[0]


def turn(x):
    y = 4.0 * (x - jnp.round(x))
    n = jnp.round(y)
    r = (0.5 * math.pi) * (y - n)
    z = r * r
    s = r + r * z * (-1.6666654611e-1 + z * (8.3321608736e-3 - 1.9515295891e-4 * z))
    c = 4.166664568298827e-2 + z * (-1.388731625493765e-3 + 2.443315711809948e-5 * z)
    c = 1.0 + z * (c * z - 0.5)
    odd = jnp.abs(n) == 1.0
    cos = jnp.where(odd, s, c)
    sin = jnp.where(odd, c, s)
    cos = jnp.where((n > 0.5) | (n < -1.5), -cos, cos)
    sin = jnp.where((n > 1.5) | (n < -0.5), -sin, sin)
    return cos, sin


def fill_powers(x, weight, low, cos_ref, sin_ref, signed):
    small = [(jnp.ones_like(x), jnp.zeros_like(x)), turn(x)]
    for b in range(2, STRIDE // 2 + 1):
        small.append(times(small[b // 2], small[b - b // 2]))
    big = times(small[-1], small[-1])

    def put(h, c, s):
        def at(r):
            return pl.ds(pl.multiple_of(r * ROWS + low, 8), HALF)

        cos_ref[at(h)] = c
        if signed:
            sin_ref[at(TOP + h)] = s
            sin_ref[at(TOP - h)] = -s
        else:
            sin_ref[at(h)] = s

    def weighted(v):
        return v if weight is None else (weight * v[0], weight * v[1])

    for b in range(STRIDE // 2):
        put(b, *weighted(small[b]))

    def around(a, state, both):
        c, s = state
        put(STRIDE * a, c, s)
        for b in range(1, STRIDE // 2 + 1):
            cb, sb = small[b]
            cc, ss, sc, cs = c * cb, s * sb, s * cb, c * sb
            put(STRIDE * a - b, cc + ss, sc - cs)
            if both and b < STRIDE // 2:
                put(STRIDE * a + b, cc - ss, sc + cs)

    def step(a, state):
        around(a, state, True)
        return times(state, big)

    last = lax.fori_loop(1, TOP // STRIDE, step, weighted(big), unroll=TOP // STRIDE - 1)
    around(TOP // STRIDE, last, False)


def eighths(v):
    return (v[0:8] + v[8:16]) + (v[16:24] + v[24:32])


def nonzero(q):
    return jnp.where(jnp.abs(q) < TINY, TINY, q)


def lines(v):
    return [v[:, at : at + 128] for at in range(0, v.shape[1], 128)]


def to_scalars(stage, scalars, sems):
    return [
        pltpu.make_async_copy(stage.at[i], scalars.at[pl.ds(128 * i, 128)], sems.at[i])
        for i in range(stage.shape[0])
    ]


def half_space(triples):
    return jnp.where(triples[0:1] < 0, -triples, triples)


def phases_kernel(
    trip_hbm, x_hbm, q_hbm, e_ref, s_ref, keep_ref, modes_ref,
    xc, xs, yc, ys, zc, zs, acc_c, acc_s, trip_ref, x_ref, q_ref, in_sems,
    xyz, stage, idx, idx_sem, ring, sems,
):
    blocks, modes = e_ref.shape[0], e_ref.shape[1]
    parts = modes // WRITE_PART
    loads = [
        pltpu.make_async_copy(src, dst, in_sems.at[i])
        for i, (src, dst) in enumerate(((x_hbm, x_ref), (q_hbm, q_ref), (trip_hbm, trip_ref)))
    ]
    for load in loads:
        load.start()

    def clear(i, carry):
        at = pl.ds(pl.multiple_of(i * 128, 128), 128)
        acc_c[at] = jnp.zeros((128, 128), jnp.float32)
        acc_s[at] = jnp.zeros((128, 128), jnp.float32)
        return carry

    lax.fori_loop(0, acc_c.shape[0] // 128, clear, 0)
    for load in loads:
        load.wait()
    triples = half_space(trip_ref[...])
    h, k, l = triples[0:1], triples[1:2], triples[2:3]
    for kind, row in enumerate((h, jnp.abs(k), k + TOP, jnp.abs(l), l + TOP)):
        for r, line in enumerate(lines(ROWS * row)):
            at = kind * (modes // 128) + r
            stage[at : at + 1] = line
    for move in to_scalars(stage, idx, idx_sem):
        move.start()
    n_lines = modes // 128
    table = [
        (2.0 * math.pi) * jnp.concatenate(lines(triples[d : d + 1]), axis=0).astype(jnp.float32)
        for d in range(3)
    ]
    norm = table[0] * table[0] + table[1] * table[1] + table[2] * table[2]
    modes_ref[:n_lines] = 4.0 * math.pi * jnp.exp(-norm / 1600000.0) / norm
    for d in range(3):
        modes_ref[n_lines * (d + 1) : n_lines * (d + 2)] = table[d]

    def fold(i, carry):
        for d in range(3):
            xyz[d, pl.ds(i, 1)] = x_ref[d : d + 1, pl.ds(pl.multiple_of(i * 128, 128), 128)]
        return carry

    lax.fori_loop(0, xyz.shape[1], fold, 0, unroll=16)
    faint = jnp.max(jnp.where(jnp.abs(q_ref[...]) < TINY, 1.0, 0.0)) > 0.0

    def copy(slot, b, p):
        return pltpu.make_async_copy(
            ring.at[slot], e_ref.at[b, pl.ds(p * WRITE_PART, WRITE_PART)], sems.at[slot]
        )

    def block(b, carry):
        for low in (0, HALF):
            here = pl.ds(pl.multiple_of(b * ROWS + low, HALF), HALF)
            for d, (c_ref, s_ref_) in enumerate(((xc, xs), (yc, ys), (zc, zs))):
                weight = nonzero(q_ref[here]) if d == 2 else None
                fill_powers(xyz[d, here], weight, low, c_ref, s_ref_, d > 0)

        @pl.when(b == 0)
        def _():
            for move in to_scalars(stage, idx, idx_sem):
                move.wait()

        def part(p, carry):
            t = b * parts + p
            slot = lax.rem(t, WRITE_SLOTS)

            @pl.when(t >= WRITE_SLOTS)
            def _():
                copy(slot, b, p).wait()

            run(ring.at[slot], b, p * WRITE_PART)
            copy(slot, b, p).start()
            return carry

        kept = jnp.where(b == blocks - 1, KEEP // WRITE_PART, 0)
        return lax.fori_loop(0, parts - kept, part, carry)

    def run(out, b, start):
        def group(g, ratio):
            sums_c, sums_s = [], []
            for j in range(GROUP):
                i = g * GROUP + j
                k = start + i
                h = idx[k]
                first = rows_of(xc, h), rows_of(xs, h)
                second = rows_of(yc, idx[modes + k]), rows_of(ys, idx[2 * modes + k])
                third = rows_of(zc, idx[3 * modes + k]), rows_of(zs, idx[4 * modes + k])
                c, s = times(times(first, second), third)
                out[i, 0] = c
                out[i, 1] = s
                if ratio is not None:
                    c, s = ratio * c, ratio * s
                sums_c.append(eighths(c))
                sums_s.append(eighths(s))
            at = pl.ds(pl.multiple_of((start + g * GROUP) * 8, 8 * GROUP), 8 * GROUP)
            sums_c = acc_c[at] + jnp.concatenate(sums_c, axis=0)
            sums_s = acc_s[at] + jnp.concatenate(sums_s, axis=0)
            acc_c[at] = sums_c
            acc_s[at] = sums_s

        groups = out.shape[0] // GROUP

        @pl.when(faint)
        def _():
            q = q_ref[pl.ds(pl.multiple_of(b * ROWS, ROWS), ROWS)]
            ratio = q / nonzero(q)
            lax.fori_loop(0, groups, lambda g, c: (group(g, ratio), c)[1], 0)

        @pl.when(jnp.logical_not(faint))
        def _():
            lax.fori_loop(
                0, groups, lambda g, c: (group(g, None), c)[1], 0, unroll=8
            )

    lax.fori_loop(0, blocks, block, 0)
    run(keep_ref, blocks - 1, modes - KEEP)

    for half, acc in enumerate((acc_c, acc_s)):
        for r in range(modes // 128):
            rows = acc[pl.ds(1024 * r, 128, stride=8)]
            for sub in range(1, 8):
                rows = rows + acc[pl.ds(1024 * r + sub, 128, stride=8)]
            at = half * (modes // 128) + r
            s_ref[at : at + 1] = jnp.sum(rows.T, axis=0, keepdims=True)

    def drain(slot, carry):
        copy(slot, 0, 0).wait()
        return carry

    lax.fori_loop(0, WRITE_SLOTS, drain, 0)


def response_kernel(scale, got_ref, modes_ref, keep_ref, e_ref, o_ref, stage, w, w_sem, ring, sems):
    blocks, modes = e_ref.shape[0], e_ref.shape[1]
    parts = modes // PART
    n_lines = modes // 128
    lead = (modes - KEEP) // PART
    n_parts = blocks * parts - KEEP // PART

    def copy(slot, b, p):
        return pltpu.make_async_copy(
            e_ref.at[b, pl.ds(p * PART, PART)], ring.at[slot], sems.at[slot]
        )

    def fetch(t):
        later = t - lead
        b = jnp.where(later < 0, blocks - 1, later // parts)
        copy(lax.rem(t, SLOTS), b, jnp.where(later < 0, t, lax.rem(later, parts))).start()

    def first(t, carry):
        fetch(t)
        return carry

    lax.fori_loop(0, SLOTS, first, 0)

    total = got_ref[0]
    for i in range(1, got_ref.shape[0]):
        total = total + got_ref[i]
    cosine, sine = total[:n_lines], total[n_lines:]
    damping = modes_ref[:n_lines]
    energy = scale * jnp.sum(damping * (cosine * cosine + sine * sine))
    stage[:n_lines] = damping * cosine
    stage[n_lines : 2 * n_lines] = damping * sine
    stage[2 * n_lines :] = modes_ref[n_lines:]
    for move in to_scalars(stage, w, w_sem):
        move.start()
    for move in to_scalars(stage, w, w_sem):
        move.wait()
    zero = jnp.zeros((ROWS, 128), jnp.float32)

    def run(source, start, state):
        def mode(i, state):
            f0, f1, f2, pot = state
            k = start + i
            wr, wi = w[k], w[modes + k]
            c = source[i, 0]
            s = source[i, 1]
            pot = pot + (wr * c + wi * s)
            g = wr * s - wi * c
            return (
                f0 + w[2 * modes + k] * g,
                f1 + w[3 * modes + k] * g,
                f2 + w[4 * modes + k] * g,
                pot,
            )

        return lax.fori_loop(0, source.shape[0], mode, state, unroll=UNROLL)

    def stream(b, before, count, state):
        def part(p, state):
            t = before + p
            slot = lax.rem(t, SLOTS)
            copy(slot, b, p).wait()
            state = run(ring.at[slot], p * PART, state)

            @pl.when(t + SLOTS < n_parts)
            def _():
                fetch(t + SLOTS)

            return state

        state = lax.fori_loop(0, count, part, state)
        for t in range(2):
            for c in range(4):
                o_ref[2 * b + t, HALF * c : HALF * (c + 1)] = state[c][HALF * t : HALF * (t + 1)]
            o_ref[2 * b + t, 4 * HALF :] = jnp.full((8, 128), energy, jnp.float32)

    stream(blocks - 1, 0, lead, run(keep_ref, modes - KEEP, (zero,) * 4))

    def block(b, carry):
        stream(b, lead + b * parts, parts, (zero,) * 4)
        return carry

    lax.fori_loop(0, blocks - 1, block, 0)


def finish_kernel(scale, sum_ref, q_ref, forces_ref, potential_ref):
    chunks = sum_ref.shape[0]

    def chunk(v, carry):
        for c in range(3):
            for r in range(HALF):
                at = pl.ds(pl.multiple_of((v * HALF + r) * 128, 128), 128)
                forces_ref[c : c + 1, at] = scale * sum_ref[v, HALF * c + r : HALF * c + r + 1]
        at = pl.ds(pl.multiple_of(v * HALF, HALF), HALF)
        potential_ref[at] = (400.0 * scale) * sum_ref[v, 3 * HALF :] / nonzero(q_ref[at])
        return carry

    lax.fori_loop(0, chunks, chunk, 0)


def on_device(scaled_coordinate_array, particle_charge_list, reciprocal_triples):
    local_atoms = scaled_coordinate_array.shape[1]
    modes = reciprocal_triples.shape[1]
    n_atom = lax.axis_size("atom")
    n_kvec = lax.axis_size("kvec")
    natoms = local_atoms * n_atom
    blocks = local_atoms // BLOCK
    n_lines = modes // 128
    q = particle_charge_list.reshape(local_atoms // 128, 128)

    vmem = pl.BlockSpec(memory_space=pltpu.VMEM)
    hbm = pl.BlockSpec(memory_space=pltpu.HBM)
    def ring(slots, part):
        return [
            pltpu.VMEM((slots, part, 2, ROWS, 128), jnp.float32),
            pltpu.SemaphoreType.DMA((slots,)),
        ]

    def scalars(dtype):
        return [
            pltpu.VMEM((KINDS * n_lines, 128), dtype),
            pltpu.SMEM((KINDS * modes,), dtype),
            pltpu.SemaphoreType.DMA((KINDS * n_lines,)),
        ]

    positive = pltpu.VMEM(((TOP + 1) * ROWS, 128), jnp.float32)
    both = pltpu.VMEM(((2 * TOP + 1) * ROWS, 128), jnp.float32)
    e, share, keep, spectrum = pl.pallas_call(
        phases_kernel,
        in_specs=[hbm, hbm, hbm],
        out_specs=[hbm, vmem, vmem, vmem],
        out_shape=[
            jax.ShapeDtypeStruct((blocks, modes, 2, ROWS, 128), jnp.float32),
            pltpu.VMEM((8, 128), jnp.float32),
            pltpu.VMEM((KEEP, 2, ROWS, 128), jnp.float32),
            pltpu.VMEM((4 * n_lines, 128), jnp.float32),
        ],
        scratch_shapes=[
            positive,
            positive,
            positive,
            both,
            positive,
            both,
            pltpu.VMEM((modes * 8, 128), jnp.float32),
            pltpu.VMEM((modes * 8, 128), jnp.float32),
            pltpu.VMEM((3, modes), jnp.int32),
            pltpu.VMEM((3, local_atoms), jnp.float32),
            pltpu.VMEM((local_atoms // 128, 128), jnp.float32),
            pltpu.SemaphoreType.DMA((3,)),
            pltpu.VMEM((3, local_atoms // 128, 128), jnp.float32),
        ]
        + scalars(jnp.int32)
        + ring(WRITE_SLOTS, WRITE_PART),
        compiler_params=pltpu.CompilerParams(vmem_limit_bytes=58 * MIB),
    )(reciprocal_triples, scaled_coordinate_array, q)

    share = share + lax.ppermute(share, "atom", [(i, i ^ 1) for i in range(n_atom)])
    share = jnp.broadcast_to(share[None], (n_atom // 2, 8, 128))
    cores = [[c + 2 * m for m in range(n_atom // 2)] for c in range(2)]
    got = lax.all_to_all(share, "atom", 0, 0, tiled=True, axis_index_groups=cores)

    terms = pl.pallas_call(
        functools.partial(response_kernel, 50.0 / natoms),
        in_specs=[vmem, vmem, vmem, hbm],
        out_specs=vmem,
        out_shape=jax.ShapeDtypeStruct((n_kvec, 4 * HALF + 8, 128), jnp.float32),
        scratch_shapes=scalars(jnp.float32) + ring(SLOTS, PART),
        compiler_params=pltpu.CompilerParams(vmem_limit_bytes=32 * MIB),
    )(got, spectrum, keep, e)

    own = lax.all_to_all(terms, "kvec", 0, 0, tiled=True).sum(axis=0)
    energy = own[4 * HALF, 0]
    copies = jnp.broadcast_to(own[None, : 4 * HALF], (n_kvec, 4 * HALF, 128))
    summed = lax.all_to_all(copies, "kvec", 0, 0, tiled=True)
    forces, potential = pl.pallas_call(
        functools.partial(finish_kernel, 1.0 / math.sqrt(natoms)),
        in_specs=[vmem, vmem],
        out_specs=[vmem, vmem],
        out_shape=[
            jax.ShapeDtypeStruct((3, local_atoms), jnp.float32),
            jax.ShapeDtypeStruct((local_atoms // 128, 128), jnp.float32),
        ],
        compiler_params=pltpu.CompilerParams(vmem_limit_bytes=8 * MIB),
    )(summed, q)
    return (forces, potential.reshape(local_atoms), energy)


def solution(mesh):
    return jax.shard_map(
        on_device,
        mesh=mesh,
        in_specs=(P(None, "atom"), P("atom"), P(None, "kvec")),
        out_specs=(P(None, "atom"), P("atom"), P()),
        check_vma=False,
    )
```

```python
import functools
import math

import jax
import jax.numpy as jnp
from jax import lax
from jax.experimental import pallas as pl
from jax.experimental.pallas import tpu as pltpu
from jax.sharding import PartitionSpec as P

TOP = 128
STRIDE = 16
BLOCK = 4096
ROWS = BLOCK // 128
HALF = ROWS // 2
PART = 32
SLOTS = 12
WRITE_PART = 64
WRITE_SLOTS = 5
KEEP = 64
UNROLL = 16
GROUP = 8
TINY = 1e-6
KINDS = 5
MIB = 1 << 20


def rows_of(ref, start):
    return ref[pl.ds(pl.multiple_of(start, ROWS), ROWS), :]


def times(a, b):
    return a[0] * b[0] - a[1] * b[1], a[0] * b[1] + a[1] * b[0]


def turn(x):
    y = 4.0 * (x - jnp.round(x))
    n = jnp.round(y)
    r = (0.5 * math.pi) * (y - n)
    z = r * r
    s = r + r * z * (-1.6666654611e-1 + z * (8.3321608736e-3 - 1.9515295891e-4 * z))
    c = 4.166664568298827e-2 + z * (-1.388731625493765e-3 + 2.443315711809948e-5 * z)
    c = 1.0 + z * (c * z - 0.5)
    odd = jnp.abs(n) == 1.0
    cos = jnp.where(odd, s, c)
    sin = jnp.where(odd, c, s)
    cos = jnp.where((n > 0.5) | (n < -1.5), -cos, cos)
    sin = jnp.where((n > 1.5) | (n < -0.5), -sin, sin)
    return cos, sin


def fill_powers(x, weight, low, cos_ref, sin_ref, signed):
    small = [(jnp.ones_like(x), jnp.zeros_like(x)), turn(x)]
    for b in range(2, STRIDE // 2 + 1):
        small.append(times(small[b // 2], small[b - b // 2]))
    big = times(small[-1], small[-1])

    def put(h, c, s):
        def at(r):
            return pl.ds(pl.multiple_of(r * ROWS + low, 8), HALF)

        cos_ref[at(h)] = c
        if signed:
            sin_ref[at(TOP + h)] = s
            sin_ref[at(TOP - h)] = -s
        else:
            sin_ref[at(h)] = s

    def weighted(v):
        return v if weight is None else (weight * v[0], weight * v[1])

    for b in range(STRIDE // 2):
        put(b, *weighted(small[b]))

    def around(a, state, both):
        c, s = state
        put(STRIDE * a, c, s)
        for b in range(1, STRIDE // 2 + 1):
            cb, sb = small[b]
            cc, ss, sc, cs = c * cb, s * sb, s * cb, c * sb
            put(STRIDE * a - b, cc + ss, sc - cs)
            if both and b < STRIDE // 2:
                put(STRIDE * a + b, cc - ss, sc + cs)

    def step(a, state):
        around(a, state, True)
        return times(state, big)

    last = lax.fori_loop(1, TOP // STRIDE, step, weighted(big), unroll=TOP // STRIDE - 1)
    around(TOP // STRIDE, last, False)


def eighths(v):
    return (v[0:8] + v[8:16]) + (v[16:24] + v[24:32])


def nonzero(q):
    return jnp.where(jnp.abs(q) < TINY, TINY, q)


def lines(v):
    return [v[:, at : at + 128] for at in range(0, v.shape[1], 128)]


def to_scalars(stage, scalars, sems):
    return [
        pltpu.make_async_copy(stage.at[i], scalars.at[pl.ds(128 * i, 128)], sems.at[i])
        for i in range(stage.shape[0])
    ]


def half_space(triples):
    return jnp.where(triples[0:1] < 0, -triples, triples)


def phases_kernel(
    trip_hbm, x_hbm, q_hbm, e_ref, s_ref, keep_ref, modes_ref,
    xc, xs, yc, ys, zc, zs, acc_c, acc_s, trip_ref, x_ref, q_ref, in_sems,
    xyz, stage, idx, idx_sem, ring, sems,
):
    blocks, modes = e_ref.shape[0], e_ref.shape[1]
    parts = modes // WRITE_PART
    loads = [
        pltpu.make_async_copy(src, dst, in_sems.at[i])
        for i, (src, dst) in enumerate(((x_hbm, x_ref), (q_hbm, q_ref), (trip_hbm, trip_ref)))
    ]
    for load in loads:
        load.start()

    def clear(i, carry):
        at = pl.ds(pl.multiple_of(i * 128, 128), 128)
        acc_c[at] = jnp.zeros((128, 128), jnp.float32)
        acc_s[at] = jnp.zeros((128, 128), jnp.float32)
        return carry

    lax.fori_loop(0, acc_c.shape[0] // 128, clear, 0)
    for load in loads:
        load.wait()
    triples = half_space(trip_ref[...])
    h, k, l = triples[0:1], triples[1:2], triples[2:3]
    for kind, row in enumerate((h, jnp.abs(k), k + TOP, jnp.abs(l), l + TOP)):
        for r, line in enumerate(lines(ROWS * row)):
            at = kind * (modes // 128) + r
            stage[at : at + 1] = line
    for move in to_scalars(stage, idx, idx_sem):
        move.start()
    n_lines = modes // 128
    table = [
        (2.0 * math.pi) * jnp.concatenate(lines(triples[d : d + 1]), axis=0).astype(jnp.float32)
        for d in range(3)
    ]
    norm = table[0] * table[0] + table[1] * table[1] + table[2] * table[2]
    modes_ref[:n_lines] = 4.0 * math.pi * jnp.exp(-norm / 1600000.0) / norm
    for d in range(3):
        modes_ref[n_lines * (d + 1) : n_lines * (d + 2)] = table[d]

    def fold(i, carry):
        for d in range(3):
            xyz[d, pl.ds(i, 1)] = x_ref[d : d + 1, pl.ds(pl.multiple_of(i * 128, 128), 128)]
        return carry

    lax.fori_loop(0, xyz.shape[1], fold, 0, unroll=16)
    faint = jnp.max(jnp.where(jnp.abs(q_ref[...]) < TINY, 1.0, 0.0)) > 0.0

    def copy(slot, b, p):
        return pltpu.make_async_copy(
            ring.at[slot], e_ref.at[b, pl.ds(p * WRITE_PART, WRITE_PART)], sems.at[slot]
        )

    def block(b, carry):
        for low in (0, HALF):
            here = pl.ds(pl.multiple_of(b * ROWS + low, HALF), HALF)
            for d, (c_ref, s_ref_) in enumerate(((xc, xs), (yc, ys), (zc, zs))):
                weight = nonzero(q_ref[here]) if d == 2 else None
                fill_powers(xyz[d, here], weight, low, c_ref, s_ref_, d > 0)

        @pl.when(b == 0)
        def _():
            for move in to_scalars(stage, idx, idx_sem):
                move.wait()

        def part(p, carry):
            t = b * parts + p
            slot = lax.rem(t, WRITE_SLOTS)

            @pl.when(t >= WRITE_SLOTS)
            def _():
                copy(slot, b, p).wait()

            run(ring.at[slot], b, p * WRITE_PART)
            copy(slot, b, p).start()
            return carry

        kept = jnp.where(b == blocks - 1, KEEP // WRITE_PART, 0)
        return lax.fori_loop(0, parts - kept, part, carry)

    def run(out, b, start):
        def group(g, ratio):
            sums_c, sums_s = [], []
            for j in range(GROUP):
                i = g * GROUP + j
                k = start + i
                h = idx[k]
                first = rows_of(xc, h), rows_of(xs, h)
                second = rows_of(yc, idx[modes + k]), rows_of(ys, idx[2 * modes + k])
                third = rows_of(zc, idx[3 * modes + k]), rows_of(zs, idx[4 * modes + k])
                c, s = times(times(first, second), third)
                out[i, 0] = c
                out[i, 1] = s
                if ratio is not None:
                    c, s = ratio * c, ratio * s
                sums_c.append(eighths(c))
                sums_s.append(eighths(s))
            at = pl.ds(pl.multiple_of((start + g * GROUP) * 8, 8 * GROUP), 8 * GROUP)
            sums_c = acc_c[at] + jnp.concatenate(sums_c, axis=0)
            sums_s = acc_s[at] + jnp.concatenate(sums_s, axis=0)
            acc_c[at] = sums_c
            acc_s[at] = sums_s

        groups = out.shape[0] // GROUP

        @pl.when(faint)
        def _():
            q = q_ref[pl.ds(pl.multiple_of(b * ROWS, ROWS), ROWS)]
            ratio = q / nonzero(q)
            lax.fori_loop(0, groups, lambda g, c: (group(g, ratio), c)[1], 0)

        @pl.when(jnp.logical_not(faint))
        def _():
            lax.fori_loop(
                0, groups, lambda g, c: (group(g, None), c)[1], 0, unroll=8
            )

    lax.fori_loop(0, blocks, block, 0)
    run(keep_ref, blocks - 1, modes - KEEP)

    for half, acc in enumerate((acc_c, acc_s)):
        for r in range(modes // 128):
            rows = acc[pl.ds(1024 * r, 128, stride=8)]
            for sub in range(1, 8):
                rows = rows + acc[pl.ds(1024 * r + sub, 128, stride=8)]
            at = half * (modes // 128) + r
            s_ref[at : at + 1] = jnp.sum(rows.T, axis=0, keepdims=True)

    def drain(slot, carry):
        copy(slot, 0, 0).wait()
        return carry

    lax.fori_loop(0, WRITE_SLOTS, drain, 0)


def response_kernel(scale, got_ref, modes_ref, keep_ref, e_ref, o_ref, stage, w, w_sem, ring, sems):
    blocks, modes = e_ref.shape[0], e_ref.shape[1]
    parts = modes // PART
    n_lines = modes // 128
    lead = (modes - KEEP) // PART
    n_parts = blocks * parts - KEEP // PART

    def copy(slot, b, p):
        return pltpu.make_async_copy(
            e_ref.at[b, pl.ds(p * PART, PART)], ring.at[slot], sems.at[slot]
        )

    def fetch(t):
        later = t - lead
        b = jnp.where(later < 0, blocks - 1, later // parts)
        copy(lax.rem(t, SLOTS), b, jnp.where(later < 0, t, lax.rem(later, parts))).start()

    def first(t, carry):
        fetch(t)
        return carry

    lax.fori_loop(0, SLOTS, first, 0)

    total = got_ref[0]
    for i in range(1, got_ref.shape[0]):
        total = total + got_ref[i]
    cosine, sine = total[:n_lines], total[n_lines:]
    damping = modes_ref[:n_lines]
    energy = scale * jnp.sum(damping * (cosine * cosine + sine * sine))
    stage[:n_lines] = damping * cosine
    stage[n_lines : 2 * n_lines] = damping * sine
    stage[2 * n_lines :] = modes_ref[n_lines:]
    for move in to_scalars(stage, w, w_sem):
        move.start()
    for move in to_scalars(stage, w, w_sem):
        move.wait()
    zero = jnp.zeros((ROWS, 128), jnp.float32)

    def run(source, start, state):
        def mode(i, state):
            f0, f1, f2, pot = state
            k = start + i
            wr, wi = w[k], w[modes + k]
            c = source[i, 0]
            s = source[i, 1]
            pot = pot + (wr * c + wi * s)
            g = wr * s - wi * c
            return (
                f0 + w[2 * modes + k] * g,
                f1 + w[3 * modes + k] * g,
                f2 + w[4 * modes + k] * g,
                pot,
            )

        return lax.fori_loop(0, source.shape[0], mode, state, unroll=UNROLL)

    def stream(b, before, count, state):
        def part(p, state):
            t = before + p
            slot = lax.rem(t, SLOTS)
            copy(slot, b, p).wait()
            state = run(ring.at[slot], p * PART, state)

            @pl.when(t + SLOTS < n_parts)
            def _():
                fetch(t + SLOTS)

            return state

        state = lax.fori_loop(0, count, part, state)
        for t in range(2):
            for c in range(4):
                o_ref[2 * b + t, HALF * c : HALF * (c + 1)] = state[c][HALF * t : HALF * (t + 1)]
            o_ref[2 * b + t, 4 * HALF :] = jnp.full((8, 128), energy, jnp.float32)

    stream(blocks - 1, 0, lead, run(keep_ref, modes - KEEP, (zero,) * 4))

    def block(b, carry):
        stream(b, lead + b * parts, parts, (zero,) * 4)
        return carry

    lax.fori_loop(0, blocks - 1, block, 0)


def gather_kernel(terms_ref, copies_ref, energy_ref):
    total = terms_ref[0]
    for i in range(1, terms_ref.shape[0]):
        total = total + terms_ref[i]
    for i in range(copies_ref.shape[0]):
        copies_ref[i] = total[: 4 * HALF]
    energy_ref[...] = total[4 * HALF :]


def finish_kernel(scale, sum_ref, q_ref, total_ref, forces_ref, potential_ref, energy_ref):
    energy_ref[0, 0] = jnp.max(total_ref[...])
    chunks = sum_ref.shape[0]

    def chunk(v, carry):
        for c in range(3):
            for r in range(HALF):
                at = pl.ds(pl.multiple_of((v * HALF + r) * 128, 128), 128)
                forces_ref[c : c + 1, at] = scale * sum_ref[v, HALF * c + r : HALF * c + r + 1]
        at = pl.ds(pl.multiple_of(v * HALF, HALF), HALF)
        potential_ref[at] = (400.0 * scale) * sum_ref[v, 3 * HALF :] / nonzero(q_ref[at])
        return carry

    lax.fori_loop(0, chunks, chunk, 0)


def on_device(scaled_coordinate_array, particle_charge_list, reciprocal_triples):
    local_atoms = scaled_coordinate_array.shape[1]
    modes = reciprocal_triples.shape[1]
    n_atom = lax.axis_size("atom")
    n_kvec = lax.axis_size("kvec")
    natoms = local_atoms * n_atom
    blocks = local_atoms // BLOCK
    n_lines = modes // 128
    q = particle_charge_list.reshape(local_atoms // 128, 128)

    vmem = pl.BlockSpec(memory_space=pltpu.VMEM)
    hbm = pl.BlockSpec(memory_space=pltpu.HBM)
    def ring(slots, part):
        return [
            pltpu.VMEM((slots, part, 2, ROWS, 128), jnp.float32),
            pltpu.SemaphoreType.DMA((slots,)),
        ]

    def scalars(dtype):
        return [
            pltpu.VMEM((KINDS * n_lines, 128), dtype),
            pltpu.SMEM((KINDS * modes,), dtype),
            pltpu.SemaphoreType.DMA((KINDS * n_lines,)),
        ]

    positive = pltpu.VMEM(((TOP + 1) * ROWS, 128), jnp.float32)
    both = pltpu.VMEM(((2 * TOP + 1) * ROWS, 128), jnp.float32)
    e, share, keep, spectrum = pl.pallas_call(
        phases_kernel,
        in_specs=[hbm, hbm, hbm],
        out_specs=[hbm, vmem, vmem, vmem],
        out_shape=[
            jax.ShapeDtypeStruct((blocks, modes, 2, ROWS, 128), jnp.float32),
            pltpu.VMEM((8, 128), jnp.float32),
            pltpu.VMEM((KEEP, 2, ROWS, 128), jnp.float32),
            pltpu.VMEM((4 * n_lines, 128), jnp.float32),
        ],
        scratch_shapes=[
            positive,
            positive,
            positive,
            both,
            positive,
            both,
            pltpu.VMEM((modes * 8, 128), jnp.float32),
            pltpu.VMEM((modes * 8, 128), jnp.float32),
            pltpu.VMEM((3, modes), jnp.int32),
            pltpu.VMEM((3, local_atoms), jnp.float32),
            pltpu.VMEM((local_atoms // 128, 128), jnp.float32),
            pltpu.SemaphoreType.DMA((3,)),
            pltpu.VMEM((3, local_atoms // 128, 128), jnp.float32),
        ]
        + scalars(jnp.int32)
        + ring(WRITE_SLOTS, WRITE_PART),
        compiler_params=pltpu.CompilerParams(vmem_limit_bytes=58 * MIB),
    )(reciprocal_triples, scaled_coordinate_array, q)

    share = share + lax.ppermute(share, "atom", [(i, i ^ 1) for i in range(n_atom)])
    share = jnp.broadcast_to(share[None], (n_atom // 2, 8, 128))
    cores = [[c + 2 * m for m in range(n_atom // 2)] for c in range(2)]
    got = lax.all_to_all(share, "atom", 0, 0, tiled=True, axis_index_groups=cores)

    terms = pl.pallas_call(
        functools.partial(response_kernel, 50.0 / natoms),
        in_specs=[vmem, vmem, vmem, hbm],
        out_specs=vmem,
        out_shape=jax.ShapeDtypeStruct((n_kvec, 4 * HALF + 8, 128), jnp.float32),
        scratch_shapes=scalars(jnp.float32) + ring(SLOTS, PART),
        compiler_params=pltpu.CompilerParams(vmem_limit_bytes=32 * MIB),
    )(got, spectrum, keep, e)

    terms = lax.all_to_all(terms, "kvec", 0, 0, tiled=True)
    copies, total = pl.pallas_call(
        gather_kernel,
        in_specs=[vmem],
        out_specs=[vmem, vmem],
        out_shape=[
            pltpu.VMEM((n_kvec, 4 * HALF, 128), jnp.float32),
            jax.ShapeDtypeStruct((8, 128), jnp.float32),
        ],
        compiler_params=pltpu.CompilerParams(vmem_limit_bytes=8 * MIB),
    )(terms)
    summed = lax.all_to_all(copies, "kvec", 0, 0, tiled=True)
    forces, potential, energy = pl.pallas_call(
        functools.partial(finish_kernel, 1.0 / math.sqrt(natoms)),
        in_specs=[vmem, vmem, vmem],
        out_specs=[vmem, vmem, pl.BlockSpec(memory_space=pltpu.SMEM)],
        out_shape=[
            jax.ShapeDtypeStruct((3, local_atoms), jnp.float32),
            jax.ShapeDtypeStruct((local_atoms // 128, 128), jnp.float32),
            jax.ShapeDtypeStruct((1, 1), jnp.float32),
        ],
        compiler_params=pltpu.CompilerParams(vmem_limit_bytes=8 * MIB),
    )(summed, q, total)
    return (forces, potential.reshape(local_atoms), energy.reshape(()))


def solution(mesh):
    return jax.shard_map(
        on_device,
        mesh=mesh,
        in_specs=(P(None, "atom"), P("atom"), P(None, "kvec")),
        out_specs=(P(None, "atom"), P("atom"), P()),
        check_vma=False,
    )
```

```python
import functools
import math

import jax
import jax.numpy as jnp
from jax import lax
from jax.experimental import pallas as pl
from jax.experimental.pallas import tpu as pltpu
from jax.sharding import PartitionSpec as P

TOP = 128
STRIDE = 16
BLOCK = 4096
ROWS = BLOCK // 128
HALF = ROWS // 2
PART = 32
SLOTS = 12
WRITE_PART = 64
WRITE_SLOTS = 5
KEEP = 64
UNROLL = 16
GROUP = 8
TINY = 1e-6
KINDS = 5
MIB = 1 << 20


def rows_of(ref, start):
    return ref[pl.ds(pl.multiple_of(start, ROWS), ROWS), :]


def times(a, b):
    return a[0] * b[0] - a[1] * b[1], a[0] * b[1] + a[1] * b[0]


def turn(x):
    y = 4.0 * (x - jnp.round(x))
    n = jnp.round(y)
    r = (0.5 * math.pi) * (y - n)
    z = r * r
    s = r + r * z * (-1.6666654611e-1 + z * (8.3321608736e-3 - 1.9515295891e-4 * z))
    c = 4.166664568298827e-2 + z * (-1.388731625493765e-3 + 2.443315711809948e-5 * z)
    c = 1.0 + z * (c * z - 0.5)
    odd = jnp.abs(n) == 1.0
    cos = jnp.where(odd, s, c)
    sin = jnp.where(odd, c, s)
    cos = jnp.where((n > 0.5) | (n < -1.5), -cos, cos)
    sin = jnp.where((n > 1.5) | (n < -0.5), -sin, sin)
    return cos, sin


def fill_powers(x, weight, low, cos_ref, sin_ref, signed):
    small = [(jnp.ones_like(x), jnp.zeros_like(x)), turn(x)]
    for b in range(2, STRIDE // 2 + 1):
        small.append(times(small[b // 2], small[b - b // 2]))
    big = times(small[-1], small[-1])

    def put(h, c, s):
        def at(r):
            return pl.ds(pl.multiple_of(r * ROWS + low, 8), HALF)

        cos_ref[at(h)] = c
        if signed:
            sin_ref[at(TOP + h)] = s
            sin_ref[at(TOP - h)] = -s
        else:
            sin_ref[at(h)] = s

    def weighted(v):
        return v if weight is None else (weight * v[0], weight * v[1])

    for b in range(STRIDE // 2):
        put(b, *weighted(small[b]))

    def around(a, state, both):
        c, s = state
        put(STRIDE * a, c, s)
        for b in range(1, STRIDE // 2 + 1):
            cb, sb = small[b]
            cc, ss, sc, cs = c * cb, s * sb, s * cb, c * sb
            put(STRIDE * a - b, cc + ss, sc - cs)
            if both and b < STRIDE // 2:
                put(STRIDE * a + b, cc - ss, sc + cs)

    def step(a, state):
        around(a, state, True)
        return times(state, big)

    last = lax.fori_loop(1, TOP // STRIDE, step, weighted(big), unroll=TOP // STRIDE - 1)
    around(TOP // STRIDE, last, False)


def eighths(v):
    return (v[0:8] + v[8:16]) + (v[16:24] + v[24:32])


def nonzero(q):
    return jnp.where(jnp.abs(q) < TINY, TINY, q)


def unfold(q):
    return jnp.where(jnp.abs(q) < TINY, q * (1.0 / TINY), 1.0)


def lines(v):
    return [v[:, at : at + 128] for at in range(0, v.shape[1], 128)]


def to_scalars(stage, scalars, sems):
    return [
        pltpu.make_async_copy(stage.at[i], scalars.at[pl.ds(128 * i, 128)], sems.at[i])
        for i in range(stage.shape[0])
    ]


def half_space(triples):
    return jnp.where(triples[0:1] < 0, -triples, triples)


def phases_kernel(
    trip_hbm, x_hbm, q_hbm, e_ref, s_ref, keep_ref, modes_ref,
    xc, xs, yc, ys, zc, zs, acc_c, acc_s, trip_ref, x_ref, q_ref, in_sems,
    xyz, stage, idx, idx_sem, ring, sems,
):
    blocks, modes = e_ref.shape[0], e_ref.shape[1]
    parts = modes // WRITE_PART
    loads = [
        pltpu.make_async_copy(src, dst, in_sems.at[i])
        for i, (src, dst) in enumerate(((x_hbm, x_ref), (q_hbm, q_ref), (trip_hbm, trip_ref)))
    ]
    for load in loads:
        load.start()

    def clear(i, carry):
        at = pl.ds(pl.multiple_of(i * 128, 128), 128)
        acc_c[at] = jnp.zeros((128, 128), jnp.float32)
        acc_s[at] = jnp.zeros((128, 128), jnp.float32)
        return carry

    lax.fori_loop(0, acc_c.shape[0] // 128, clear, 0)
    for load in loads:
        load.wait()
    triples = half_space(trip_ref[...])
    h, k, l = triples[0:1], triples[1:2], triples[2:3]
    for kind, row in enumerate((h, jnp.abs(k), k + TOP, jnp.abs(l), l + TOP)):
        for r, line in enumerate(lines(ROWS * row)):
            at = kind * (modes // 128) + r
            stage[at : at + 1] = line
    for move in to_scalars(stage, idx, idx_sem):
        move.start()
    n_lines = modes // 128
    table = [
        (2.0 * math.pi) * jnp.concatenate(lines(triples[d : d + 1]), axis=0).astype(jnp.float32)
        for d in range(3)
    ]
    norm = table[0] * table[0] + table[1] * table[1] + table[2] * table[2]
    modes_ref[:n_lines] = 4.0 * math.pi * jnp.exp(-norm / 1600000.0) / norm
    for d in range(3):
        modes_ref[n_lines * (d + 1) : n_lines * (d + 2)] = table[d]

    def fold(i, carry):
        for d in range(3):
            xyz[d, pl.ds(i, 1)] = x_ref[d : d + 1, pl.ds(pl.multiple_of(i * 128, 128), 128)]
        return carry

    lax.fori_loop(0, xyz.shape[1], fold, 0, unroll=16)
    faint = jnp.max(jnp.where(jnp.abs(q_ref[...]) < TINY, 1.0, 0.0)) > 0.0

    def copy(slot, b, p):
        return pltpu.make_async_copy(
            ring.at[slot], e_ref.at[b, pl.ds(p * WRITE_PART, WRITE_PART)], sems.at[slot]
        )

    def block(b, carry):
        for low in (0, HALF):
            here = pl.ds(pl.multiple_of(b * ROWS + low, HALF), HALF)
            for d, (c_ref, s_ref_) in enumerate(((xc, xs), (yc, ys), (zc, zs))):
                weight = nonzero(q_ref[here]) if d == 2 else None
                fill_powers(xyz[d, here], weight, low, c_ref, s_ref_, d > 0)

        @pl.when(b == 0)
        def _():
            for move in to_scalars(stage, idx, idx_sem):
                move.wait()

        def part(p, carry):
            t = b * parts + p
            slot = lax.rem(t, WRITE_SLOTS)

            @pl.when(t >= WRITE_SLOTS)
            def _():
                copy(slot, b, p).wait()

            run(ring.at[slot], b, p * WRITE_PART)
            copy(slot, b, p).start()
            return carry

        kept = jnp.where(b == blocks - 1, KEEP // WRITE_PART, 0)
        return lax.fori_loop(0, parts - kept, part, carry)

    def run(out, b, start):
        def group(g, ratio):
            sums_c, sums_s = [], []
            for j in range(GROUP):
                i = g * GROUP + j
                k = start + i
                h = idx[k]
                first = rows_of(xc, h), rows_of(xs, h)
                second = rows_of(yc, idx[modes + k]), rows_of(ys, idx[2 * modes + k])
                third = rows_of(zc, idx[3 * modes + k]), rows_of(zs, idx[4 * modes + k])
                c, s = times(times(first, second), third)
                out[i, 0] = c
                out[i, 1] = s
                if ratio is not None:
                    c, s = ratio * c, ratio * s
                sums_c.append(eighths(c))
                sums_s.append(eighths(s))
            at = pl.ds(pl.multiple_of((start + g * GROUP) * 8, 8 * GROUP), 8 * GROUP)
            sums_c = acc_c[at] + jnp.concatenate(sums_c, axis=0)
            sums_s = acc_s[at] + jnp.concatenate(sums_s, axis=0)
            acc_c[at] = sums_c
            acc_s[at] = sums_s

        groups = out.shape[0] // GROUP

        @pl.when(faint)
        def _():
            q = q_ref[pl.ds(pl.multiple_of(b * ROWS, ROWS), ROWS)]
            ratio = unfold(q)
            lax.fori_loop(0, groups, lambda g, c: (group(g, ratio), c)[1], 0)

        @pl.when(jnp.logical_not(faint))
        def _():
            lax.fori_loop(
                0, groups, lambda g, c: (group(g, None), c)[1], 0, unroll=8
            )

    lax.fori_loop(0, blocks, block, 0)
    run(keep_ref, blocks - 1, modes - KEEP)

    for half, acc in enumerate((acc_c, acc_s)):
        for r in range(modes // 128):
            rows = acc[pl.ds(1024 * r, 128, stride=8)]
            for sub in range(1, 8):
                rows = rows + acc[pl.ds(1024 * r + sub, 128, stride=8)]
            at = half * (modes // 128) + r
            s_ref[at : at + 1] = jnp.sum(rows.T, axis=0, keepdims=True)

    def drain(slot, carry):
        copy(slot, 0, 0).wait()
        return carry

    lax.fori_loop(0, WRITE_SLOTS, drain, 0)


def response_kernel(scale, got_ref, modes_ref, keep_ref, e_ref, o_ref, stage, w, w_sem, ring, sems):
    blocks, modes = e_ref.shape[0], e_ref.shape[1]
    parts = modes // PART
    n_lines = modes // 128
    lead = (modes - KEEP) // PART
    n_parts = blocks * parts - KEEP // PART

    def copy(slot, b, p):
        return pltpu.make_async_copy(
            e_ref.at[b, pl.ds(p * PART, PART)], ring.at[slot], sems.at[slot]
        )

    def fetch(t):
        later = t - lead
        b = jnp.where(later < 0, blocks - 1, later // parts)
        copy(lax.rem(t, SLOTS), b, jnp.where(later < 0, t, lax.rem(later, parts))).start()

    def first(t, carry):
        fetch(t)
        return carry

    lax.fori_loop(0, SLOTS, first, 0)

    total = got_ref[0]
    for i in range(1, got_ref.shape[0]):
        total = total + got_ref[i]
    cosine, sine = total[:n_lines], total[n_lines:]
    damping = modes_ref[:n_lines]
    energy = scale * jnp.sum(damping * (cosine * cosine + sine * sine))
    stage[:n_lines] = damping * cosine
    stage[n_lines : 2 * n_lines] = damping * sine
    stage[2 * n_lines :] = modes_ref[n_lines:]
    for move in to_scalars(stage, w, w_sem):
        move.start()
    for move in to_scalars(stage, w, w_sem):
        move.wait()
    zero = jnp.zeros((ROWS, 128), jnp.float32)

    def run(source, start, state):
        def mode(i, state):
            f0, f1, f2, pot = state
            k = start + i
            wr, wi = w[k], w[modes + k]
            c = source[i, 0]
            s = source[i, 1]
            pot = pot + (wr * c + wi * s)
            g = wr * s - wi * c
            return (
                f0 + w[2 * modes + k] * g,
                f1 + w[3 * modes + k] * g,
                f2 + w[4 * modes + k] * g,
                pot,
            )

        return lax.fori_loop(0, source.shape[0], mode, state, unroll=UNROLL)

    def stream(b, before, count, state):
        def part(p, state):
            t = before + p
            slot = lax.rem(t, SLOTS)
            copy(slot, b, p).wait()
            state = run(ring.at[slot], p * PART, state)

            @pl.when(t + SLOTS < n_parts)
            def _():
                fetch(t + SLOTS)

            return state

        state = lax.fori_loop(0, count, part, state)
        for t in range(2):
            for c in range(4):
                o_ref[2 * b + t, HALF * c : HALF * (c + 1)] = state[c][HALF * t : HALF * (t + 1)]
            o_ref[2 * b + t, 4 * HALF :] = jnp.full((8, 128), energy, jnp.float32)

    stream(blocks - 1, 0, lead, run(keep_ref, modes - KEEP, (zero,) * 4))

    def block(b, carry):
        stream(b, lead + b * parts, parts, (zero,) * 4)
        return carry

    lax.fori_loop(0, blocks - 1, block, 0)


def gather_kernel(terms_ref, copies_ref, energy_ref):
    total = terms_ref[0]
    for i in range(1, terms_ref.shape[0]):
        total = total + terms_ref[i]
    for i in range(copies_ref.shape[0]):
        copies_ref[i] = total[: 4 * HALF]
    energy_ref[...] = total[4 * HALF :]


def finish_kernel(scale, sum_ref, q_ref, total_ref, forces_ref, potential_ref, energy_ref):
    energy_ref[0, 0] = jnp.max(total_ref[...])
    chunks = sum_ref.shape[0]

    def chunk(v, carry):
        for r in range(HALF):
            at = pl.ds(pl.multiple_of((v * HALF + r) * 128, 128), 128)
            factor = scale * unfold(q_ref[pl.ds(v * HALF + r, 1)])
            for c in range(3):
                forces_ref[c : c + 1, at] = factor * sum_ref[v, HALF * c + r : HALF * c + r + 1]
        at = pl.ds(pl.multiple_of(v * HALF, HALF), HALF)
        potential_ref[at] = (400.0 * scale) * sum_ref[v, 3 * HALF :] / nonzero(q_ref[at])
        return carry

    lax.fori_loop(0, chunks, chunk, 0)


def on_device(scaled_coordinate_array, particle_charge_list, reciprocal_triples):
    local_atoms = scaled_coordinate_array.shape[1]
    modes = reciprocal_triples.shape[1]
    n_atom = lax.axis_size("atom")
    n_kvec = lax.axis_size("kvec")
    natoms = local_atoms * n_atom
    blocks = local_atoms // BLOCK
    n_lines = modes // 128
    q = particle_charge_list.reshape(local_atoms // 128, 128)

    vmem = pl.BlockSpec(memory_space=pltpu.VMEM)
    hbm = pl.BlockSpec(memory_space=pltpu.HBM)
    def ring(slots, part):
        return [
            pltpu.VMEM((slots, part, 2, ROWS, 128), jnp.float32),
            pltpu.SemaphoreType.DMA((slots,)),
        ]

    def scalars(dtype):
        return [
            pltpu.VMEM((KINDS * n_lines, 128), dtype),
            pltpu.SMEM((KINDS * modes,), dtype),
            pltpu.SemaphoreType.DMA((KINDS * n_lines,)),
        ]

    positive = pltpu.VMEM(((TOP + 1) * ROWS, 128), jnp.float32)
    both = pltpu.VMEM(((2 * TOP + 1) * ROWS, 128), jnp.float32)
    e, share, keep, spectrum = pl.pallas_call(
        phases_kernel,
        in_specs=[hbm, hbm, hbm],
        out_specs=[hbm, vmem, vmem, vmem],
        out_shape=[
            jax.ShapeDtypeStruct((blocks, modes, 2, ROWS, 128), jnp.float32),
            pltpu.VMEM((8, 128), jnp.float32),
            pltpu.VMEM((KEEP, 2, ROWS, 128), jnp.float32),
            pltpu.VMEM((4 * n_lines, 128), jnp.float32),
        ],
        scratch_shapes=[
            positive,
            positive,
            positive,
            both,
            positive,
            both,
            pltpu.VMEM((modes * 8, 128), jnp.float32),
            pltpu.VMEM((modes * 8, 128), jnp.float32),
            pltpu.VMEM((3, modes), jnp.int32),
            pltpu.VMEM((3, local_atoms), jnp.float32),
            pltpu.VMEM((local_atoms // 128, 128), jnp.float32),
            pltpu.SemaphoreType.DMA((3,)),
            pltpu.VMEM((3, local_atoms // 128, 128), jnp.float32),
        ]
        + scalars(jnp.int32)
        + ring(WRITE_SLOTS, WRITE_PART),
        compiler_params=pltpu.CompilerParams(vmem_limit_bytes=58 * MIB),
    )(reciprocal_triples, scaled_coordinate_array, q)

    share = share + lax.ppermute(share, "atom", [(i, i ^ 1) for i in range(n_atom)])
    share = jnp.broadcast_to(share[None], (n_atom // 2, 8, 128))
    cores = [[c + 2 * m for m in range(n_atom // 2)] for c in range(2)]
    got = lax.all_to_all(share, "atom", 0, 0, tiled=True, axis_index_groups=cores)

    terms = pl.pallas_call(
        functools.partial(response_kernel, 50.0 / natoms),
        in_specs=[vmem, vmem, vmem, hbm],
        out_specs=vmem,
        out_shape=jax.ShapeDtypeStruct((n_kvec, 4 * HALF + 8, 128), jnp.float32),
        scratch_shapes=scalars(jnp.float32) + ring(SLOTS, PART),
        compiler_params=pltpu.CompilerParams(vmem_limit_bytes=32 * MIB),
    )(got, spectrum, keep, e)

    terms = lax.all_to_all(terms, "kvec", 0, 0, tiled=True)
    copies, total = pl.pallas_call(
        gather_kernel,
        in_specs=[vmem],
        out_specs=[vmem, vmem],
        out_shape=[
            pltpu.VMEM((n_kvec, 4 * HALF, 128), jnp.float32),
            jax.ShapeDtypeStruct((8, 128), jnp.float32),
        ],
        compiler_params=pltpu.CompilerParams(vmem_limit_bytes=8 * MIB),
    )(terms)
    summed = lax.all_to_all(copies, "kvec", 0, 0, tiled=True)
    forces, potential, energy = pl.pallas_call(
        functools.partial(finish_kernel, 1.0 / math.sqrt(natoms)),
        in_specs=[vmem, vmem, vmem],
        out_specs=[vmem, vmem, pl.BlockSpec(memory_space=pltpu.SMEM)],
        out_shape=[
            jax.ShapeDtypeStruct((3, local_atoms), jnp.float32),
            jax.ShapeDtypeStruct((local_atoms // 128, 128), jnp.float32),
            jax.ShapeDtypeStruct((1, 1), jnp.float32),
        ],
        compiler_params=pltpu.CompilerParams(vmem_limit_bytes=8 * MIB),
    )(summed, q, total)
    return (forces, potential.reshape(local_atoms), energy.reshape(()))


def solution(mesh):
    return jax.shard_map(
        on_device,
        mesh=mesh,
        in_specs=(P(None, "atom"), P("atom"), P(None, "kvec")),
        out_specs=(P(None, "atom"), P("atom"), P()),
        check_vma=False,
    )
```

```python
import functools
import math

import jax
import jax.numpy as jnp
from jax import lax
from jax.experimental import pallas as pl
from jax.experimental.pallas import tpu as pltpu
from jax.sharding import PartitionSpec as P

TOP = 128
STRIDE = 16
BLOCK = 4096
ROWS = BLOCK // 128
HALF = ROWS // 2
PART = 32
SLOTS = 12
WRITE_PART = 64
WRITE_SLOTS = 5
KEEP = 64
UNROLL = 16
GROUP = 8
TINY = 1e-6
KINDS = 5
MIB = 1 << 20


def rows_of(ref, start):
    return ref[pl.ds(pl.multiple_of(start, ROWS), ROWS), :]


def times(a, b):
    return a[0] * b[0] - a[1] * b[1], a[0] * b[1] + a[1] * b[0]


def turn(x):
    y = 4.0 * (x - jnp.round(x))
    n = jnp.round(y)
    r = (0.5 * math.pi) * (y - n)
    z = r * r
    s = r + r * z * (-1.6666654611e-1 + z * (8.3321608736e-3 - 1.9515295891e-4 * z))
    c = 4.166664568298827e-2 + z * (-1.388731625493765e-3 + 2.443315711809948e-5 * z)
    c = 1.0 + z * (c * z - 0.5)
    odd = jnp.abs(n) == 1.0
    cos = jnp.where(odd, s, c)
    sin = jnp.where(odd, c, s)
    cos = jnp.where((n > 0.5) | (n < -1.5), -cos, cos)
    sin = jnp.where((n > 1.5) | (n < -0.5), -sin, sin)
    return cos, sin


def fill_powers(x, weight, low, cos_ref, sin_ref, signed):
    small = [(jnp.ones_like(x), jnp.zeros_like(x)), turn(x)]
    for b in range(2, STRIDE // 2 + 1):
        small.append(times(small[b // 2], small[b - b // 2]))
    big = times(small[-1], small[-1])

    def put(h, c, s):
        def at(r):
            return pl.ds(pl.multiple_of(r * ROWS + low, 8), HALF)

        cos_ref[at(h)] = c
        if signed:
            sin_ref[at(TOP + h)] = s
            sin_ref[at(TOP - h)] = -s
        else:
            sin_ref[at(h)] = s

    def weighted(v):
        return v if weight is None else (weight * v[0], weight * v[1])

    for b in range(STRIDE // 2):
        put(b, *weighted(small[b]))

    def around(a, state, both):
        c, s = state
        put(STRIDE * a, c, s)
        for b in range(1, STRIDE // 2 + 1):
            cb, sb = small[b]
            cc, ss, sc, cs = c * cb, s * sb, s * cb, c * sb
            put(STRIDE * a - b, cc + ss, sc - cs)
            if both and b < STRIDE // 2:
                put(STRIDE * a + b, cc - ss, sc + cs)

    def step(a, state):
        around(a, state, True)
        return times(state, big)

    last = lax.fori_loop(1, TOP // STRIDE, step, weighted(big), unroll=TOP // STRIDE - 1)
    around(TOP // STRIDE, last, False)


def eighths(v):
    return (v[0:8] + v[8:16]) + (v[16:24] + v[24:32])


def nonzero(q):
    return jnp.where(jnp.abs(q) < TINY, TINY, q)


def unfold(q):
    return jnp.where(jnp.abs(q) < TINY, q * (1.0 / TINY), 1.0)


def lines(v):
    return [v[:, at : at + 128] for at in range(0, v.shape[1], 128)]


def to_scalars(stage, scalars, sems):
    return [
        pltpu.make_async_copy(stage.at[i], scalars.at[pl.ds(128 * i, 128)], sems.at[i])
        for i in range(sems.shape[0])
    ]


def half_space(triples):
    return jnp.where(triples[0:1] < 0, -triples, triples)


def phases_kernel(
    trip_hbm, x_hbm, q_hbm, e_ref, s_ref, keep_ref, modes_ref,
    xc, xs, yc, ys, zc, zs, acc_c, acc_s, trip_ref, x_ref, q_ref, in_sems,
    xyz, stage, idx, idx_sem, ring, sems,
):
    blocks, modes = e_ref.shape[0], e_ref.shape[1]
    parts = modes // WRITE_PART
    loads = [
        pltpu.make_async_copy(src, dst, in_sems.at[i])
        for i, (src, dst) in enumerate(((x_hbm, x_ref), (q_hbm, q_ref), (trip_hbm, trip_ref)))
    ]
    for load in loads:
        load.start()

    def clear(i, carry):
        at = pl.ds(pl.multiple_of(i * 128, 128), 128)
        acc_c[at] = jnp.zeros((128, 128), jnp.float32)
        acc_s[at] = jnp.zeros((128, 128), jnp.float32)
        return carry

    lax.fori_loop(0, acc_c.shape[0] // 128, clear, 0)
    for load in loads:
        load.wait()
    triples = half_space(trip_ref[...])
    h, k, l = triples[0:1], triples[1:2], triples[2:3]
    for kind, row in enumerate((h, jnp.abs(k), k + TOP, jnp.abs(l), l + TOP)):
        for r, line in enumerate(lines(ROWS * row)):
            at = kind * (modes // 128) + r
            stage[at : at + 1] = line
    for move in to_scalars(stage, idx, idx_sem):
        move.start()
    n_lines = modes // 128
    table = [
        (2.0 * math.pi) * jnp.concatenate(lines(triples[d : d + 1]), axis=0).astype(jnp.float32)
        for d in range(3)
    ]
    norm = table[0] * table[0] + table[1] * table[1] + table[2] * table[2]
    modes_ref[:n_lines] = 4.0 * math.pi * jnp.exp(-norm / 1600000.0) / norm
    for d in range(3):
        modes_ref[n_lines * (d + 1) : n_lines * (d + 2)] = table[d]

    def fold(i, carry):
        for d in range(3):
            xyz[d, pl.ds(i, 1)] = x_ref[d : d + 1, pl.ds(pl.multiple_of(i * 128, 128), 128)]
        return carry

    lax.fori_loop(0, xyz.shape[1], fold, 0, unroll=16)
    faint = jnp.max(jnp.where(jnp.abs(q_ref[...]) < TINY, 1.0, 0.0)) > 0.0

    def copy(slot, b, p):
        return pltpu.make_async_copy(
            ring.at[slot], e_ref.at[b, pl.ds(p * WRITE_PART, WRITE_PART)], sems.at[slot]
        )

    def block(b, carry):
        for low in (0, HALF):
            here = pl.ds(pl.multiple_of(b * ROWS + low, HALF), HALF)
            for d, (c_ref, s_ref_) in enumerate(((xc, xs), (yc, ys), (zc, zs))):
                weight = nonzero(q_ref[here]) if d == 2 else None
                fill_powers(xyz[d, here], weight, low, c_ref, s_ref_, d > 0)

        @pl.when(b == 0)
        def _():
            for move in to_scalars(stage, idx, idx_sem):
                move.wait()

        def part(p, carry):
            t = b * parts + p
            slot = lax.rem(t, WRITE_SLOTS)

            @pl.when(t >= WRITE_SLOTS)
            def _():
                copy(slot, b, p).wait()

            run(ring.at[slot], b, p * WRITE_PART)
            copy(slot, b, p).start()
            return carry

        kept = jnp.where(b == blocks - 1, KEEP // WRITE_PART, 0)
        return lax.fori_loop(0, parts - kept, part, carry)

    def run(out, b, start):
        def group(g, ratio):
            sums_c, sums_s = [], []
            for j in range(GROUP):
                i = g * GROUP + j
                k = start + i
                h = idx[k]
                first = rows_of(xc, h), rows_of(xs, h)
                second = rows_of(yc, idx[modes + k]), rows_of(ys, idx[2 * modes + k])
                third = rows_of(zc, idx[3 * modes + k]), rows_of(zs, idx[4 * modes + k])
                c, s = times(times(first, second), third)
                out[i, 0] = c
                out[i, 1] = s
                if ratio is not None:
                    c, s = ratio * c, ratio * s
                sums_c.append(eighths(c))
                sums_s.append(eighths(s))
            at = pl.ds(pl.multiple_of((start + g * GROUP) * 8, 8 * GROUP), 8 * GROUP)
            sums_c = acc_c[at] + jnp.concatenate(sums_c, axis=0)
            sums_s = acc_s[at] + jnp.concatenate(sums_s, axis=0)
            acc_c[at] = sums_c
            acc_s[at] = sums_s

        groups = out.shape[0] // GROUP

        @pl.when(faint)
        def _():
            q = q_ref[pl.ds(pl.multiple_of(b * ROWS, ROWS), ROWS)]
            ratio = unfold(q)
            lax.fori_loop(0, groups, lambda g, c: (group(g, ratio), c)[1], 0)

        @pl.when(jnp.logical_not(faint))
        def _():
            lax.fori_loop(
                0, groups, lambda g, c: (group(g, None), c)[1], 0, unroll=8
            )

    lax.fori_loop(0, blocks, block, 0)
    run(keep_ref, blocks - 1, modes - KEEP)

    for half, acc in enumerate((acc_c, acc_s)):
        for r in range(modes // 128):
            rows = acc[pl.ds(1024 * r, 128, stride=8)]
            for sub in range(1, 8):
                rows = rows + acc[pl.ds(1024 * r + sub, 128, stride=8)]
            at = half * (modes // 128) + r
            s_ref[at : at + 1] = jnp.sum(rows.T, axis=0, keepdims=True)

    def drain(slot, carry):
        copy(slot, 0, 0).wait()
        return carry

    lax.fori_loop(0, WRITE_SLOTS, drain, 0)


def response_kernel(scale, got_ref, modes_ref, keep_ref, e_ref, o_ref, stage, w, w_sem, ring, sems):
    blocks, modes = e_ref.shape[0], e_ref.shape[1]
    parts = modes // PART
    n_lines = modes // 128
    lead = (modes - KEEP) // PART
    n_parts = blocks * parts - KEEP // PART

    def copy(slot, b, p):
        return pltpu.make_async_copy(
            e_ref.at[b, pl.ds(p * PART, PART)], ring.at[slot], sems.at[slot]
        )

    def fetch(t):
        later = t - lead
        b = jnp.where(later < 0, blocks - 1, later // parts)
        copy(lax.rem(t, SLOTS), b, jnp.where(later < 0, t, lax.rem(later, parts))).start()

    def first(t, carry):
        fetch(t)
        return carry

    lax.fori_loop(0, SLOTS, first, 0)

    total = got_ref[0]
    for i in range(1, got_ref.shape[0]):
        total = total + got_ref[i]
    cosine, sine = total[:n_lines], total[n_lines:]
    damping = modes_ref[:n_lines]
    energy = scale * jnp.sum(damping * (cosine * cosine + sine * sine))
    stage[:n_lines] = damping * cosine
    stage[n_lines : 2 * n_lines] = damping * sine
    stage[2 * n_lines : 5 * n_lines] = modes_ref[n_lines:]
    for move in to_scalars(stage, w, w_sem):
        move.start()
    for move in to_scalars(stage, w, w_sem):
        move.wait()
    zero = jnp.zeros((ROWS, 128), jnp.float32)

    def run(source, start, state):
        def mode(i, state):
            f0, f1, f2, pot = state
            k = start + i
            wr, wi = w[k], w[modes + k]
            c = source[i, 0]
            s = source[i, 1]
            pot = pot + (wr * c + wi * s)
            g = wr * s - wi * c
            return (
                f0 + w[2 * modes + k] * g,
                f1 + w[3 * modes + k] * g,
                f2 + w[4 * modes + k] * g,
                pot,
            )

        return lax.fori_loop(0, source.shape[0], mode, state, unroll=UNROLL)

    def stream(b, before, count, state):
        def part(p, state):
            t = before + p
            slot = lax.rem(t, SLOTS)
            copy(slot, b, p).wait()
            state = run(ring.at[slot], p * PART, state)

            @pl.when(t + SLOTS < n_parts)
            def _():
                fetch(t + SLOTS)

            return state

        state = lax.fori_loop(0, count, part, state)
        for t in range(2):
            for c in range(4):
                o_ref[2 * b + t, HALF * c : HALF * (c + 1)] = state[c][HALF * t : HALF * (t + 1)]
            o_ref[2 * b + t, 4 * HALF :] = jnp.full((8, 128), energy, jnp.float32)

    stream(blocks - 1, 0, lead, run(keep_ref, modes - KEEP, (zero,) * 4))

    def block(b, carry):
        stream(b, lead + b * parts, parts, (zero,) * 4)
        return carry

    lax.fori_loop(0, blocks - 1, block, 0)


def gather_kernel(terms_ref, copies_ref, energy_ref):
    total = terms_ref[0]
    for i in range(1, terms_ref.shape[0]):
        total = total + terms_ref[i]
    for i in range(copies_ref.shape[0]):
        copies_ref[i] = total[: 4 * HALF]
    energy_ref[...] = total[4 * HALF :]


def finish_kernel(scale, sum_ref, q_ref, total_ref, forces_ref, potential_ref, energy_ref):
    energy_ref[0, 0] = jnp.max(total_ref[...])
    chunks = sum_ref.shape[0]

    def chunk(v, carry):
        for r in range(HALF):
            at = pl.ds(pl.multiple_of((v * HALF + r) * 128, 128), 128)
            factor = scale * unfold(q_ref[pl.ds(v * HALF + r, 1)])
            for c in range(3):
                forces_ref[c : c + 1, at] = factor * sum_ref[v, HALF * c + r : HALF * c + r + 1]
        at = pl.ds(pl.multiple_of(v * HALF, HALF), HALF)
        potential_ref[at] = (400.0 * scale) * sum_ref[v, 3 * HALF :] / nonzero(q_ref[at])
        return carry

    lax.fori_loop(0, chunks, chunk, 0)


def on_device(scaled_coordinate_array, particle_charge_list, reciprocal_triples):
    local_atoms = scaled_coordinate_array.shape[1]
    modes = reciprocal_triples.shape[1]
    n_atom = lax.axis_size("atom")
    n_kvec = lax.axis_size("kvec")
    natoms = local_atoms * n_atom
    blocks = local_atoms // BLOCK
    n_lines = modes // 128
    q = particle_charge_list.reshape(local_atoms // 128, 128)

    vmem = pl.BlockSpec(memory_space=pltpu.VMEM)
    hbm = pl.BlockSpec(memory_space=pltpu.HBM)
    def ring(slots, part):
        return [
            pltpu.VMEM((slots, part, 2, ROWS, 128), jnp.float32),
            pltpu.SemaphoreType.DMA((slots,)),
        ]

    def scalars(dtype):
        return [
            pltpu.VMEM((pl.cdiv(KINDS * n_lines, 8) * 8, 128), dtype),
            pltpu.SMEM((KINDS * modes,), dtype),
            pltpu.SemaphoreType.DMA((KINDS * n_lines,)),
        ]

    positive = pltpu.VMEM(((TOP + 1) * ROWS, 128), jnp.float32)
    both = pltpu.VMEM(((2 * TOP + 1) * ROWS, 128), jnp.float32)
    e, share, keep, spectrum = pl.pallas_call(
        phases_kernel,
        in_specs=[hbm, hbm, hbm],
        out_specs=[hbm, vmem, vmem, vmem],
        out_shape=[
            jax.ShapeDtypeStruct((blocks, modes, 2, ROWS, 128), jnp.float32),
            pltpu.VMEM((8, 128), jnp.float32),
            pltpu.VMEM((KEEP, 2, ROWS, 128), jnp.float32),
            pltpu.VMEM((4 * n_lines, 128), jnp.float32),
        ],
        scratch_shapes=[
            positive,
            positive,
            positive,
            both,
            positive,
            both,
            pltpu.VMEM((modes * 8 + 8, 128), jnp.float32),
            pltpu.VMEM((modes * 8 + 8, 128), jnp.float32),
            pltpu.VMEM((3, modes), jnp.int32),
            pltpu.VMEM((3, local_atoms), jnp.float32),
            pltpu.VMEM((local_atoms // 128, 128), jnp.float32),
            pltpu.SemaphoreType.DMA((3,)),
            pltpu.VMEM((3, local_atoms // 128, 128), jnp.float32),
        ]
        + scalars(jnp.int32)
        + ring(WRITE_SLOTS, WRITE_PART),
        compiler_params=pltpu.CompilerParams(vmem_limit_bytes=58 * MIB),
    )(reciprocal_triples, scaled_coordinate_array, q)

    share = share + lax.ppermute(share, "atom", [(i, i ^ 1) for i in range(n_atom)])
    share = jnp.broadcast_to(share[None], (n_atom // 2, 8, 128))
    cores = [[c + 2 * m for m in range(n_atom // 2)] for c in range(2)]
    got = lax.all_to_all(share, "atom", 0, 0, tiled=True, axis_index_groups=cores)

    terms = pl.pallas_call(
        functools.partial(response_kernel, 50.0 / natoms),
        in_specs=[vmem, vmem, vmem, hbm],
        out_specs=vmem,
        out_shape=jax.ShapeDtypeStruct((n_kvec, 4 * HALF + 8, 128), jnp.float32),
        scratch_shapes=scalars(jnp.float32) + ring(SLOTS, PART),
        compiler_params=pltpu.CompilerParams(vmem_limit_bytes=32 * MIB),
    )(got, spectrum, keep, e)

    terms = lax.all_to_all(terms, "kvec", 0, 0, tiled=True)
    copies, total = pl.pallas_call(
        gather_kernel,
        in_specs=[vmem],
        out_specs=[vmem, vmem],
        out_shape=[
            pltpu.VMEM((n_kvec, 4 * HALF, 128), jnp.float32),
            jax.ShapeDtypeStruct((8, 128), jnp.float32),
        ],
        compiler_params=pltpu.CompilerParams(vmem_limit_bytes=8 * MIB),
    )(terms)
    summed = lax.all_to_all(copies, "kvec", 0, 0, tiled=True)
    forces, potential, energy = pl.pallas_call(
        functools.partial(finish_kernel, 1.0 / math.sqrt(natoms)),
        in_specs=[vmem, vmem, vmem],
        out_specs=[vmem, vmem, pl.BlockSpec(memory_space=pltpu.SMEM)],
        out_shape=[
            jax.ShapeDtypeStruct((3, local_atoms), jnp.float32),
            jax.ShapeDtypeStruct((local_atoms // 128, 128), jnp.float32),
            jax.ShapeDtypeStruct((1, 1), jnp.float32),
        ],
        compiler_params=pltpu.CompilerParams(vmem_limit_bytes=8 * MIB),
    )(summed, q, total)
    return (forces, potential.reshape(local_atoms), energy.reshape(()))


def solution(mesh):
    return jax.shard_map(
        on_device,
        mesh=mesh,
        in_specs=(P(None, "atom"), P("atom"), P(None, "kvec")),
        out_specs=(P(None, "atom"), P("atom"), P()),
        check_vma=False,
    )
```
